128 devices in a mesh: dp: 16 (over x, y), tensor: 8 (over z, core).
Axes of the slice: x: 4, y: 4, z: 4, core: 2. Of those that a mesh axis runs over, the one named last changes fastest.
Arguments:
- tokens: bfloat16 [256, 5376], P('dp'), may hold values from -6 to 6
- lengths: int32 [256], P('dp'), may hold values from 1 to 1024, as said below
- positions: int32 [256], P('dp'), may hold values from 1 to 33791, as said below
- in_gain: float32 [5376], replicated, may hold values from 0.25 to 1.75
- q_weight: bfloat16 [5376, 4096], P('dp', 'tensor'), may hold values from -0.078125 to 0.078125
- k_weight: bfloat16 [5376, 2048], P('dp', 'tensor'), may hold values from -0.078125 to 0.078125
- v_weight: bfloat16 [5376, 2048], P('dp', 'tensor'), may hold values from -0.078125 to 0.078125
- q_gain: float32 [128], replicated, may hold values from 0.1 to 1.9
- k_gain: float32 [128], replicated, may hold values from 0.1 to 1.9
- key_cache: bfloat16 [256, 1024, 2048], P('dp', None, 'tensor'), may hold values from -480 to 480
- value_cache: bfloat16 [256, 1024, 2048], P('dp', None, 'tensor'), may hold values from -6 to 6
- out_weight: bfloat16 [4096, 5376], P('tensor', 'dp'), may hold values from -0.09375 to 0.09375
- post_gain: float32 [5376], replicated, may hold values from 0.25 to 1.75
Outputs:
- hidden_out: bfloat16 [256, 5376], P('dp')
- new_keys: bfloat16 [256, 2048], P('dp', 'tensor')
- new_values: bfloat16 [256, 2048], P('dp', 'tensor')
The draws below stay inside these ranges and needn't reach their ends.
Inputs may be any that keep to these rules, and one draw needn't show every extreme that they name: Slots 0 to lengths - 1 of a sequence hold its cache; some sequence has exactly 1024. `positions`: each position is at least the sequence's length.
All inputs are finite; a program needn't handle non-finite values.
Results may differ from the reference program's by a relative error of at most 0.012.
The reference program's roundings to bfloat16 on the way count: a program that leaves them out, or rounds other values in their place, can miss the bound.
Values may be sent and summed in bfloat16 or wider, within the bound.
A program may use at most 64 MiB of HBM per device.

```python
import jax
import jax.numpy as jnp
from jax import lax

D = 5376
H = 32
KV = 16
HD = 128
QPRE = 168
BSEQ = 16
CTX = 1024
BATCH = 256


def length_table(key):
    groups = BATCH // BSEQ
    key_one, key_two, key_three, key_four = jax.random.split(jax.random.fold_in(key, 7), 4)
    ceiling = jax.random.randint(key_one, (groups, 1), max(CTX // 8, 1), CTX + 1)
    raw_draws = jax.random.randint(key_two, (groups, BSEQ), 0, 1 << 30)
    filled = (1 + raw_draws % ceiling).reshape(BATCH)
    chosen = jax.random.randint(key_three, (), 0, BATCH)
    filled = jnp.where(jnp.arange(BATCH) == chosen, CTX, filled)
    shifts = jax.random.randint(key_four, (BATCH,), 0, 32768)
    return (filled.astype(jnp.int32), (filled + shifts).astype(jnp.int32))


def draw_lengths(key, part):
    return length_table(key)[0]


def draw_positions(key, part):
    return length_table(key)[1]


def draw_key_cache(key, part):
    key_one, key_two = jax.random.split(jax.random.fold_in(key, 13))
    normal = 3.0 * jax.random.truncated_normal(key_one, -4.0, 4.0, (BATCH, CTX, KV * HD), jnp.float32)
    return normal.astype(jnp.bfloat16)


def steps_of(stream_key, shape, cuts, least, top_value):
    level = 1.0
    for axis_at, blocks in cuts:
        heights = jax.random.uniform(jax.random.fold_in(jax.random.fold_in(stream_key, 6), axis_at), (blocks,), jnp.float32, least / len(cuts), top_value / len(cuts))
        level = level * jnp.repeat(jnp.exp(heights), shape[axis_at] // blocks).reshape((-1,) + (1,) * (len(shape) - 1 - axis_at))
    return level


def noise(key, extent, width, limit, shards=(), held_as=jnp.bfloat16):
    entries = width * jax.random.normal(key, extent, jnp.float32)
    if shards:
        entries = entries * steps_of(key, extent, shards, -0.22, 0.18)
    return jnp.clip(entries, -limit, limit).astype(held_as)


def setup_inputs(seed: int = 0) -> dict:
    arg_keys = jax.random.split(jax.random.key(seed), 14)
    tokens = noise(arg_keys[0], (BATCH, D), 1.0, 6.0, ((0, 16),))
    lengths = draw_lengths(jax.random.fold_in(arg_keys[13], 71), 0)
    positions = draw_positions(jax.random.fold_in(arg_keys[13], 71), 0)
    in_gain = jnp.clip(1.0 + 0.15 * jax.random.normal(arg_keys[3], (D,), jnp.float32), 0.25, 1.75)
    q_weight = noise(arg_keys[4], (D, H * HD), D ** -0.5, 0.078125, ((0, 16), (1, 8)))
    k_weight = noise(arg_keys[5], (D, KV * HD), D ** -0.5, 0.078125, ((0, 16), (1, 8)))
    v_weight = noise(arg_keys[6], (D, KV * HD), D ** -0.5, 0.078125, ((0, 16), (1, 8)))
    q_gain = jnp.clip(1.0 + 0.18 * jax.random.normal(arg_keys[7], (HD,), jnp.float32), 0.1, 1.9)
    k_gain = jnp.clip(1.0 + 0.18 * jax.random.normal(arg_keys[8], (HD,), jnp.float32), 0.1, 1.9)
    key_cache = draw_key_cache(jax.random.fold_in(arg_keys[13], 71), 0)
    value_cache = noise(arg_keys[10], (BATCH, CTX, KV * HD), 1.0, 6.0, ((0, 16), (2, 8)))
    out_weight = noise(arg_keys[11], (H * HD, D), (H * HD) ** -0.5, 0.09375, ((0, 8), (1, 16)))
    post_gain = jnp.clip(1.0 + 0.15 * jax.random.normal(arg_keys[12], (D,), jnp.float32), 0.25, 1.75)
    return dict(tokens=tokens, lengths=lengths, positions=positions, in_gain=in_gain, q_weight=q_weight, k_weight=k_weight, v_weight=v_weight, q_gain=q_gain, k_gain=k_gain, key_cache=key_cache, value_cache=value_cache, out_weight=out_weight, post_gain=post_gain)


epsilon = 1e-06
rope_base = 1000000.0
rope_factor = 8.0

def rms_scale(vectors, gain):
    mean_square = lax.optimization_barrier(jnp.mean(vectors * vectors, axis=-1, keepdims=True))
    return vectors * lax.rsqrt(mean_square + epsilon) * gain

def rotate(vectors, positions):
    half_width = vectors.shape[-1] // 2
    exponent = jnp.arange(half_width, dtype=jnp.float32) * (2.0 / vectors.shape[-1])
    frequency = jnp.power(rope_base, -exponent)
    angles = (positions.astype(jnp.float32) / rope_factor)[:, None] * frequency[None, :]
    cos_part = jnp.cos(angles)[:, None, :]
    sin_part = jnp.sin(angles)[:, None, :]
    first_half = vectors[..., :half_width]
    second_half = vectors[..., half_width:]
    return jnp.concatenate([first_half * cos_part - second_half * sin_part, second_half * cos_part + first_half * sin_part], axis=-1)

def reference(tokens, lengths, positions, in_gain, q_weight, k_weight, v_weight, q_gain, k_gain, key_cache, value_cache, out_weight, post_gain):
    batch_size = tokens.shape[0]
    per_group = H // KV
    normed = rms_scale(tokens.astype(jnp.float32), in_gain).astype(jnp.bfloat16)
    q_raw = jnp.dot(normed, q_weight, preferred_element_type=jnp.float32).reshape(batch_size, H, HD)
    k_raw = jnp.dot(normed, k_weight, preferred_element_type=jnp.float32).reshape(batch_size, KV, HD)
    v_raw = jnp.dot(normed, v_weight, preferred_element_type=jnp.float32)
    new_values = v_raw.astype(jnp.bfloat16)
    queries = (rotate(rms_scale(q_raw, q_gain), positions) * QPRE ** (-0.5)).astype(jnp.bfloat16)
    new_keys = rotate(rms_scale(k_raw, k_gain), positions).astype(jnp.bfloat16).reshape(batch_size, KV * HD)

    def attend(sequence):
        query_row, key_own, value_own, cache_keys, cache_values, length = sequence
        grouped = query_row.astype(jnp.float32).reshape(KV, per_group, HD)
        keys_f = cache_keys.astype(jnp.float32).reshape(CTX, KV, HD)
        values_f = cache_values.astype(jnp.float32).reshape(CTX, KV, HD)
        scores = jnp.einsum('grd,jgd->grj', grouped, keys_f)
        usable = jnp.arange(CTX) < length
        scores = jnp.where(usable[None, None, :], scores, -jnp.inf)
        self_score = jnp.einsum('grd,gd->gr', grouped, key_own.astype(jnp.float32).reshape(KV, HD))
        largest = jnp.maximum(lax.optimization_barrier(jnp.max(scores, axis=-1)), self_score)
        weights = jnp.exp(scores - largest[..., None])
        self_weight = jnp.exp(self_score - largest)
        running = lax.optimization_barrier(jnp.sum(weights, axis=-1)) + self_weight
        rounded = lax.optimization_barrier(weights.astype(jnp.bfloat16)).astype(jnp.float32)
        rounded_self = lax.optimization_barrier(self_weight.astype(jnp.bfloat16)).astype(jnp.float32)
        mixture = jnp.einsum('grj,jgd->grd', rounded, values_f)
        mixture = mixture + rounded_self[..., None] * value_own.astype(jnp.float32).reshape(KV, 1, HD)
        return (mixture / running[..., None]).reshape(H * HD).astype(jnp.bfloat16)
    attended = lax.map(attend, (queries, new_keys, new_values, key_cache, value_cache, lengths))
    projected = jnp.dot(attended, out_weight, preferred_element_type=jnp.float32)
    hidden_out = (tokens.astype(jnp.float32) + rms_scale(projected, post_gain)).astype(jnp.bfloat16)
    return (hidden_out, new_keys, new_values)
```

```python
import functools

import jax
import jax.numpy as jnp
import numpy as np
from jax import lax
from jax.experimental import pallas as pl
from jax.experimental.pallas import tpu as pltpu
from jax.sharding import PartitionSpec as P

HD = 128
QPRE = 168
LANES = 128
EPS = 1e-06
ROPE_BASE = 1000000.0
ROPE_FACTOR = 8.0
MESH = pl.DeviceIdType.MESH
F32 = jnp.float32
BF16 = jnp.bfloat16


def padded(width):
    return -(-width // LANES) * LANES


def ring_distance(step, size):
    return min(step % size, -step % size)


def plane_offsets(side):
    steps = [(a, b) for a in range(side) for b in range(side)]
    return sorted(steps, key=lambda s: (ring_distance(s[0], side) + ring_distance(s[1], side), s))


def line_offsets(depth):
    steps = [(a, c) for a in range(depth) for c in range(2)]
    return sorted(steps, key=lambda s: (ring_distance(s[0], depth), s[1]))


def kernel(
    dims,
    tokens_hbm, lengths_hbm, positions_hbm, in_gain_hbm, qw_hbm, kw_hbm, vw_hbm, q_gain_hbm, k_gain_hbm,
    kc_hbm, vc_hbm, ow_hbm, post_gain_hbm, freq_hbm,
    hid_hbm, nk_out, nv_out,
    tokens, lengths, positions, in_gain, weights, q_gain, k_gain, kcache, vcache, oweight, post_gain, freq,
    normed, tok_mine, slots, spread, part_out, part_in, scores, probs, att_in, prod, red_out, red_in,
    proj_out, proj_in, row_out,
    load_sem, cache_sem, s1, r1, s2, r2, s3, r3, s4, r4, s5, r5, s6, r6, last_sem,
):
    dp, tensor, side, rows, width, share, q_cols, kv_cols, ctx = dims
    depth = tensor // 2
    mine = rows // tensor
    heads = q_cols // HD
    kv_heads = kv_cols // HD
    per_kv = heads // kv_heads
    share_pad = padded(share)
    me = lax.axis_index("dp")
    me_t = lax.axis_index("tensor")
    my_x, my_y = me // side, me % side
    my_z, my_c = me_t // 2, me_t % 2

    def plane_peer(step):
        return ((my_x + step[0]) % side) * side + (my_y + step[1]) % side

    def plane_source(step):
        return ((my_x + side - step[0]) % side) * side + (my_y + side - step[1]) % side

    def line_peer(step):
        return ((my_z + step[0]) % depth) * 2 + (my_c + step[1]) % 2

    plane = plane_offsets(side)
    line = line_offsets(depth)

    def load(src, dst, at):
        copy = pltpu.make_async_copy(src, dst, load_sem.at[at])
        copy.start()
        return copy

    c_tokens = load(tokens_hbm, tokens, 0)
    c_gain = load(in_gain_hbm, in_gain, 1)
    c_w = [
        load(qw_hbm, weights.at[pl.ds(0, share), pl.ds(0, q_cols)], 2),
        load(kw_hbm, weights.at[pl.ds(0, share), pl.ds(q_cols, kv_cols)], 3),
        load(vw_hbm, weights.at[pl.ds(0, share), pl.ds(q_cols + kv_cols, kv_cols)], 4),
    ]
    c_small = [
        load(lengths_hbm, lengths, 5), load(positions_hbm, positions, 6), load(q_gain_hbm, q_gain, 7),
        load(k_gain_hbm, k_gain, 8), load(post_gain_hbm, post_gain, 9), load(freq_hbm, freq, 10),
    ]
    c_ow = load(ow_hbm, oweight, 11)

    barrier = pltpu.get_barrier_semaphore()
    for step in plane[1:]:
        pl.semaphore_signal(barrier, inc=1, device_id={"dp": plane_peer(step)}, device_id_type=MESH)
    for step in line[1:]:
        pl.semaphore_signal(barrier, inc=1, device_id={"tensor": line_peer(step)}, device_id_type=MESH)

    c_k, c_v = [], []
    for b in range(rows):
        copy = pltpu.make_async_copy(kc_hbm.at[b], kcache.at[b], cache_sem.at[0, b])
        copy.start()
        c_k.append(copy)
    for b in range(rows):
        copy = pltpu.make_async_copy(vc_hbm.at[b], vcache.at[b], cache_sem.at[1, b])
        copy.start()
        c_v.append(copy)

    c_tokens.wait()
    c_gain.wait()
    x = tokens[...].astype(F32)
    mean_square = jnp.sum(x * x, axis=1, keepdims=True) * (1.0 / width)
    normed[:, :width] = x * lax.rsqrt(mean_square + EPS) * in_gain[...]
    normed[:, width:] = jnp.zeros((rows, normed.shape[1] - width), F32)
    for d in range(dp):
        first = share * d
        low = first // LANES * LANES
        window = normed[:, low : low + share_pad + LANES]
        if first != low:
            window = pltpu.roll(window, window.shape[1] - (first - low), 1)
        slots[d] = window[:, :share_pad].astype(BF16)

    pl.semaphore_wait(barrier, len(plane) + len(line) - 2)

    sends = []

    def send(src, dst, send_sem, recv_sem, device):
        copy = pltpu.make_async_remote_copy(
            src_ref=src, dst_ref=dst, send_sem=send_sem, recv_sem=recv_sem, device_id=device, device_id_type=MESH
        )
        copy.start()
        sends.append(copy)
        return copy

    first_copies = [None] * dp
    for k in range(1, dp):
        peer = plane_peer(plane[k])
        first_copies[k] = send(slots.at[peer], spread.at[k], s1.at[k], r1.at[k], {"dp": peer})
    spread[0] = slots[me]

    weights[share:, :] = jnp.zeros((share_pad - share, weights.shape[1]), BF16)
    for copy in c_small:
        copy.wait()
    sub = lax.broadcasted_iota(jnp.int32, (rows, rows), 0)
    lane = lax.broadcasted_iota(jnp.int32, (rows, rows), 1)
    pos_col = jnp.sum(jnp.where(sub == lane, positions[...].astype(F32), 0.0), axis=1, keepdims=True)
    angles = (pos_col * (1.0 / ROPE_FACTOR)) * freq[...]
    cos_part = jnp.cos(angles)
    half = lax.broadcasted_iota(jnp.int32, (rows, HD), 1) < HD // 2
    sin_part = jnp.where(half, -jnp.sin(angles), jnp.sin(angles))
    len_row = jnp.concatenate([lengths[...]] * heads + [jnp.zeros((1, HD // 2 - heads * rows), jnp.int32)] * (heads * rows < HD // 2), axis=1)
    len_row = jnp.concatenate([len_row, len_row], axis=1)
    own_rows = lax.broadcasted_iota(jnp.int32, (rows, LANES), 0)
    for tile in range(width // LANES):
        block = tokens[:, tile * LANES : (tile + 1) * LANES].astype(F32)
        for i in range(mine):
            tok_mine[i : i + 1, tile * LANES : (tile + 1) * LANES] = jnp.sum(
                jnp.where(own_rows == me_t * mine + i, block, 0.0), axis=0, keepdims=True
            )
    for copy in c_w:
        copy.wait()

    group = max(dp // 4, 1)
    own_part = None
    second_copies = [None] * dp
    for g0 in range(0, dp, group):
        for k in range(max(g0, 1), g0 + group):
            first_copies[k].wait_recv()
        lhs = spread[g0 : g0 + group].reshape(group * rows, share_pad)
        part = jnp.dot(lhs, weights[...], preferred_element_type=F32)
        if g0 == 0:
            own_part = part[:rows]
        part_out[g0 : g0 + group] = part.astype(BF16).reshape(group, rows, part.shape[1])
        for k in range(max(g0, 1), g0 + group):
            second_copies[k] = send(
                part_out.at[k], part_in.at[k], s2.at[k], r2.at[k], {"dp": plane_source(plane[k])}
            )

    joined = own_part
    for k in range(1, dp):
        second_copies[k].wait_recv()
        joined = joined + part_in[k].astype(F32)

    def rms_rope(vectors, gain):
        square = jnp.sum(vectors * vectors, axis=1, keepdims=True) * (1.0 / HD)
        scaled = vectors * lax.rsqrt(square + EPS) * gain
        return scaled * cos_part + pltpu.roll(scaled, HD // 2, 1) * sin_part

    queries = [
        (rms_rope(joined[:, h * HD : (h + 1) * HD], q_gain[...]) * QPRE ** (-0.5)).astype(BF16) for h in range(heads)
    ]
    new_keys = jnp.concatenate(
        [rms_rope(joined[:, q_cols + g * HD : q_cols + (g + 1) * HD], k_gain[...]) for g in range(kv_heads)], axis=1
    ).astype(BF16)
    new_values = joined[:, q_cols + kv_cols :].astype(BF16)
    nk_out[...] = new_keys
    nv_out[...] = new_values

    zero_head = jnp.zeros((rows, HD), BF16)
    stacked = [
        jnp.concatenate([queries[h] if g == h // per_kv else zero_head for g in range(kv_heads)], axis=1)
        for h in range(heads)
    ]
    used = heads * rows
    if used < HD // 2:
        stacked.append(jnp.zeros((HD // 2 - used, kv_cols), BF16))
    query_rows = jnp.concatenate(stacked, axis=0)
    half_rows = HD // 2
    query_of = lax.broadcasted_iota(jnp.int32, (half_rows, 1), 0) % rows
    zeros_half = jnp.zeros((half_rows, kv_cols), BF16)
    picks = [(query_of == b).astype(F32).astype(BF16) for b in range(rows)]
    contract_last = (((1,), (1,)), ((), ()))
    for copy in c_k:
        copy.wait()
    slots_half = ctx // 2
    block_rows = min(256, slots_half)
    blocks = slots_half // block_rows
    low_q, high_q = [], []
    for b in range(rows):
        only = query_rows * picks[b]
        low_q.append(jnp.concatenate([only, zeros_half], axis=0))
        high_q.append(jnp.concatenate([zeros_half, only], axis=0))
    lane_row = lax.broadcasted_iota(jnp.int32, (1, HD), 1)
    base_slot = jnp.where(lane_row < half_rows, 0, slots_half)
    largest = None
    for m in range(blocks):
        total = None
        for b in range(rows):
            low = lax.dot_general(
                kcache[b, m * block_rows : (m + 1) * block_rows, :], low_q[b], contract_last, preferred_element_type=F32
            )
            high = lax.dot_general(
                kcache[b, slots_half + m * block_rows : slots_half + (m + 1) * block_rows, :], high_q[b],
                contract_last, preferred_element_type=F32,
            )
            total = low + high if total is None else total + low + high
        slot = lax.broadcasted_iota(jnp.int32, (block_rows, HD), 0) + (m * block_rows) + base_slot
        total = jnp.where(slot < len_row, total, -jnp.inf)
        scores[m * block_rows : (m + 1) * block_rows, :] = total
        top = jnp.max(total, axis=0, keepdims=True)
        largest = top if largest is None else jnp.maximum(largest, top)
    own_scores = lax.dot_general(
        new_keys, jnp.concatenate([query_rows, query_rows], axis=0), contract_last, preferred_element_type=F32
    )
    own_lane = lax.broadcasted_iota(jnp.int32, (rows, HD), 1) % rows
    own_diag = lax.broadcasted_iota(jnp.int32, (rows, HD), 0) == own_lane
    own_row = jnp.sum(jnp.where(own_diag, own_scores, 0.0), axis=0, keepdims=True)
    largest = jnp.maximum(jnp.maximum(largest, pltpu.roll(largest, half_rows, 1)), own_row)
    own_weight = jnp.exp(own_row - largest)
    total_row = None
    for m in range(blocks):
        weight = jnp.exp(scores[m * block_rows : (m + 1) * block_rows, :] - largest)
        part_total = jnp.sum(weight, axis=0, keepdims=True)
        total_row = part_total if total_row is None else total_row + part_total
        probs[:, m * block_rows : (m + 1) * block_rows] = weight.T.astype(BF16)
    total_row = total_row + pltpu.roll(total_row, half_rows, 1) + own_weight
    eye = lax.broadcasted_iota(jnp.int32, (half_rows, HD), 0) == lax.broadcasted_iota(jnp.int32, (half_rows, HD), 1)
    total_col = jnp.sum(jnp.where(eye, total_row, 0.0), axis=1, keepdims=True)
    own_block = jnp.where(own_diag, own_weight, 0.0)[:, :half_rows].astype(BF16)
    mixture = lax.dot_general(own_block, new_values, (((0,), (0,)), ((), ())), preferred_element_type=F32)
    for copy in c_v:
        copy.wait()
    low_p = probs[:half_rows, :]
    high_p = probs[half_rows:, :]
    for b in range(rows):
        mixture = mixture + jnp.dot(low_p * picks[b], vcache[b, :slots_half, :], preferred_element_type=F32)
        mixture = mixture + jnp.dot(high_p * picks[b], vcache[b, slots_half:, :], preferred_element_type=F32)
    mixture = mixture / total_col
    attended = jnp.concatenate(
        [mixture[h * rows : (h + 1) * rows, (h // per_kv) * HD : (h // per_kv + 1) * HD] for h in range(heads)], axis=1
    ).astype(BF16)

    att_in[0] = attended
    third_copies = [None] * dp
    for k in range(1, dp):
        third_copies[k] = send(att_in.at[0], att_in.at[k], s3.at[k], r3.at[k], {"dp": plane_peer(plane[k])})
    c_ow.wait()
    for k in range(1, dp):
        third_copies[k].wait_recv()
    products = lax.dot_general(
        att_in[...].reshape(dp * rows, q_cols), oweight[...], contract_last, preferred_element_type=F32
    )
    products = jnp.concatenate([products, jnp.zeros((dp * rows, share_pad - share), F32)], axis=1)
    for c in range(share_pad // LANES):
        prod[c] = products[:, c * LANES : (c + 1) * LANES]

    for t in range(tensor):
        for i in range(mine):
            for c in range(share_pad // LANES):
                red_out[t, i, :, c * LANES : (c + 1) * LANES] = prod[c, pl.ds(mine * t + i, dp, rows), :].astype(BF16)
    fourth_copies = [None] * tensor
    for k in range(1, tensor):
        peer = line_peer(line[k])
        fourth_copies[k] = send(red_out.at[peer], red_in.at[k], s4.at[k], r4.at[k], {"tensor": peer})
    red_in[0] = red_out[me_t]
    for k in range(1, tensor):
        fourth_copies[k].wait_recv()
    shift = lax.rem(me * share, LANES)
    lanes_of = lax.broadcasted_iota(jnp.int32, (dp, LANES), 1)
    for i in range(mine):
        summed = red_in[0, i].astype(F32)
        for k in range(1, tensor):
            summed = summed + red_in[k, i].astype(F32)
        turned = [
            pltpu.roll(summed[:, c * LANES : (c + 1) * LANES], shift, 1) for c in range(share_pad // LANES)
        ]
        none = jnp.zeros((dp, LANES), F32)
        window = jnp.concatenate(
            [jnp.where(lanes_of < shift, before, after) for before, after in zip([none] + turned, turned + [none])],
            axis=1,
        )
        for k in range(dp):
            proj_out[k, i : i + 1, :] = window[k : k + 1, :]

    fifth_copies = [None] * dp
    for k in range(1, dp):
        fifth_copies[k] = send(
            proj_out.at[k], proj_in.at[me], s5.at[k], r5.at[k], {"dp": plane_source(plane[k])}
        )
    proj_in[me] = proj_out[0]
    for k in range(1, dp):
        fifth_copies[k].wait_recv()
    tiles = [jnp.zeros((mine, LANES), F32) for _ in range(width // LANES)]
    for d in range(dp):
        first = share * d
        low = first // LANES
        for c in range((first + share - 1) // LANES - low + 1):
            tiles[low + c] = tiles[low + c] + proj_in[d, :, c * LANES : (c + 1) * LANES]
    square = tiles[0] * tiles[0]
    for tile in tiles[1:]:
        square = square + tile * tile
    scale = lax.rsqrt(jnp.sum(square, axis=1, keepdims=True) * (1.0 / width) + EPS)
    projected = jnp.concatenate(tiles, axis=1)
    row_out[...] = (tok_mine[...] + projected * scale * post_gain[...]).astype(BF16)

    keep = pltpu.make_async_copy(row_out, hid_hbm.at[me_t], last_sem)
    keep.start()
    sixth_copies = [None] * tensor
    for k in range(1, tensor):
        sixth_copies[k] = send(
            row_out, hid_hbm.at[me_t], s6.at[k], r6.at[k], {"tensor": line_peer(line[k])}
        )
    for k in range(1, tensor):
        sixth_copies[k].wait_recv()
    keep.wait()
    for copy in sends:
        copy.wait_send()


def per_device(dp, tensor, side, *args):
    tokens, lengths, positions, in_gain, qw, kw, vw, q_gain, k_gain, kc, vc, ow, post_gain = args
    rows, width = tokens.shape
    share, q_cols = qw.shape
    kv_cols = kw.shape[1]
    ctx = kc.shape[1]
    share_pad = padded(share)
    cols = q_cols + 2 * kv_cols
    mine = rows // tensor
    dims = (dp, tensor, side, rows, width, share, q_cols, kv_cols, ctx)
    exponent = np.arange(HD // 2, dtype=np.float64) * (2.0 / HD)
    frequency = (ROPE_BASE**-exponent).astype(np.float32)
    freq = jnp.asarray(np.concatenate([frequency, frequency])[None])
    any_spec = pl.BlockSpec(memory_space=pl.ANY)
    vmem_spec = pl.BlockSpec(memory_space=pltpu.VMEM)
    dma = pltpu.SemaphoreType.DMA
    hidden, new_keys, new_values = pl.pallas_call(
        functools.partial(kernel, dims),
        out_shape=(
            jax.ShapeDtypeStruct((tensor, mine, width), BF16),
            jax.ShapeDtypeStruct((rows, kv_cols), BF16),
            jax.ShapeDtypeStruct((rows, kv_cols), BF16),
        ),
        in_specs=[any_spec] * 14,
        out_specs=(any_spec, vmem_spec, vmem_spec),
        scratch_shapes=[
            pltpu.VMEM((rows, width), BF16),
            pltpu.VMEM((1, rows), jnp.int32),
            pltpu.VMEM((1, rows), jnp.int32),
            pltpu.VMEM((1, width), F32),
            pltpu.VMEM((share_pad, cols), BF16),
            pltpu.VMEM((1, HD), F32),
            pltpu.VMEM((1, HD), F32),
            pltpu.VMEM((rows, ctx, kv_cols), BF16),
            pltpu.VMEM((rows, ctx, kv_cols), BF16),
            pltpu.VMEM((share, q_cols), BF16),
            pltpu.VMEM((1, width), F32),
            pltpu.VMEM((1, HD), F32),
            pltpu.VMEM((rows, width + 2 * LANES), F32),
            pltpu.VMEM((mine, width), F32),
            pltpu.VMEM((dp, rows, share_pad), BF16),
            pltpu.VMEM((dp, rows, share_pad), BF16),
            pltpu.VMEM((dp, rows, cols), BF16),
            pltpu.VMEM((dp, rows, cols), BF16),
            pltpu.VMEM((ctx // 2, HD), F32),
            pltpu.VMEM((HD, ctx // 2), BF16),
            pltpu.VMEM((dp, rows, q_cols), BF16),
            pltpu.VMEM((share_pad // LANES, dp * rows, LANES), F32),
            pltpu.VMEM((tensor, mine, dp, share_pad), BF16),
            pltpu.VMEM((tensor, mine, dp, share_pad), BF16),
            pltpu.VMEM((dp, mine, share_pad + LANES), F32),
            pltpu.VMEM((dp, mine, share_pad + LANES), F32),
            pltpu.VMEM((mine, width), BF16),
            dma((12,)),
            dma((2, rows)),
            dma((dp,)), dma((dp,)),
            dma((dp,)), dma((dp,)),
            dma((dp,)), dma((dp,)),
            dma((tensor,)), dma((tensor,)),
            dma((dp,)), dma((dp,)),
            dma((tensor,)), dma((tensor,)),
            dma(()),
        ],
        compiler_params=pltpu.CompilerParams(collective_id=0, has_side_effects=True),
    )(
        tokens, lengths.reshape(1, rows), positions.reshape(1, rows), in_gain.reshape(1, width), qw, kw, vw,
        q_gain.reshape(1, HD), k_gain.reshape(1, HD), kc, vc, ow.T, post_gain.reshape(1, width), freq,
    )
    return hidden.reshape(rows, width), new_keys, new_values


def solution(mesh):
    dp, tensor = mesh.shape["dp"], mesh.shape["tensor"]
    side = int(round(dp**0.5))
    return jax.shard_map(
        functools.partial(per_device, dp, tensor, side),
        mesh=mesh,
        in_specs=(
            P("dp", None), P("dp"), P("dp"), P(), P("dp", "tensor"), P("dp", "tensor"), P("dp", "tensor"), P(), P(),
            P("dp", None, "tensor"), P("dp", None, "tensor"), P("tensor", "dp"), P(),
        ),
        out_specs=(P("dp", None), P("dp", "tensor"), P("dp", "tensor")),
        check_vma=False,
    )
```

```python
import functools

import jax
import jax.numpy as jnp
import numpy as np
from jax import lax
from jax.experimental import pallas as pl
from jax.experimental.pallas import tpu as pltpu
from jax.sharding import PartitionSpec as P

HD = 128
QPRE = 168
LANES = 128
EPS = 1e-06
ROPE_BASE = 1000000.0
ROPE_FACTOR = 8.0
MESH = pl.DeviceIdType.MESH
F32 = jnp.float32
BF16 = jnp.bfloat16


def padded(width):
    return -(-width // LANES) * LANES


def ring_distance(step, size):
    return min(step % size, -step % size)


def plane_offsets(side):
    steps = [(a, b) for a in range(side) for b in range(side)]
    return sorted(steps, key=lambda s: (ring_distance(s[0], side) + ring_distance(s[1], side), s))


def line_offsets(depth):
    steps = [(a, c) for a in range(depth) for c in range(2)]
    return sorted(steps, key=lambda s: (ring_distance(s[0], depth), s[1]))


def kernel(
    dims,
    tokens_hbm, lengths_hbm, positions_hbm, in_gain_hbm, qw_hbm, kw_hbm, vw_hbm, q_gain_hbm, k_gain_hbm,
    kc_hbm, vc_hbm, ow_hbm, post_gain_hbm, freq_hbm,
    hid_hbm, nk_out, nv_out,
    tokens, lengths, positions, in_gain, weights, q_gain, k_gain, kcache, vcache, oweight, post_gain, freq,
    normed, tok_mine, slots, spread, part_out, part_in, scores, probs, att_in, red_out, red_in, row_out,
    load_sem, cache_sem, s1, r1, s2, r2, s3, r3, s4, r4, s5, r5, sw, rw, last_sem,
):
    dp, tensor, side, rows, width, share, q_cols, kv_cols, ctx, strip = dims
    depth = tensor // 2
    mine = rows // tensor
    heads = q_cols // HD
    kv_heads = kv_cols // HD
    per_kv = heads // kv_heads
    share_pad = padded(share)
    me = lax.axis_index("dp")
    me_t = lax.axis_index("tensor")
    my_x, my_y = lax.div(me, side), lax.rem(me, side)
    my_z, my_c = lax.div(me_t, 2), lax.rem(me_t, 2)
    xs = [my_x] + [lax.rem(my_x + a, side) for a in range(1, side)]
    ys = [my_y] + [lax.rem(my_y + a, side) for a in range(1, side)]
    zs = [my_z] + [lax.rem(my_z + a, depth) for a in range(1, depth)]
    cs = [my_c, 1 - my_c]

    def plane_peer(step):
        return xs[step[0]] * side + ys[step[1]]

    def plane_source(step):
        return xs[-step[0]] * side + ys[-step[1]]

    def line_peer(step):
        return zs[step[0]] * 2 + cs[step[1]]

    plane = plane_offsets(side)
    line = line_offsets(depth)
    ring = sorted(range(side), key=lambda a: (ring_distance(a, side), a))

    skew = lax.rem(my_x * (side * share), LANES)
    edge = strip - side * share
    oweight[:edge, :] = jnp.zeros((edge, q_cols), BF16)
    oweight[side * share :, :] = jnp.zeros((edge, q_cols), BF16)

    barrier = pltpu.get_barrier_semaphore()
    for step in reversed(plane[1:]):
        pl.semaphore_signal(barrier, inc=1, device_id={"dp": plane_peer(step)}, device_id_type=MESH)
    for kx, ahead in enumerate(ring):
        for kt, step in enumerate(line):
            if kt:
                pl.semaphore_signal(
                    barrier, inc=1, device_id={"dp": plane_peer((ahead, 0)), "tensor": line_peer(step)},
                    device_id_type=MESH,
                )

    def load(src, dst, at):
        copy = pltpu.make_async_copy(src, dst, load_sem.at[at])
        copy.start()
        return copy

    c_tokens = load(tokens_hbm, tokens, 0)
    c_gain = load(in_gain_hbm, in_gain.at[0], 1)
    c_w = [
        load(qw_hbm, weights.at[pl.ds(0, share), pl.ds(0, q_cols)], 2),
        load(kw_hbm, weights.at[pl.ds(0, share), pl.ds(q_cols, kv_cols)], 3),
        load(vw_hbm, weights.at[pl.ds(0, share), pl.ds(q_cols + kv_cols, kv_cols)], 4),
    ]
    c_small = [
        load(lengths_hbm, lengths, 5), load(positions_hbm, positions, 6), load(q_gain_hbm, q_gain, 7),
        load(k_gain_hbm, k_gain, 8), load(post_gain_hbm, post_gain.at[0], 9), load(freq_hbm, freq, 10),
    ]
    def rows_of(y, first, count):
        return oweight.at[pl.ds(pl.multiple_of(skew + y * share + first, 16), count), :]

    own_block = rows_of(my_y, 0, share)
    c_ow = load(ow_hbm, own_block, 11)

    c_tokens.wait()
    c_gain.wait()
    x = tokens[...].astype(F32)
    mean_square = jnp.sum(x * x, axis=1, keepdims=True) * (1.0 / width)
    normed[:, :width] = x * lax.rsqrt(mean_square + EPS) * in_gain[...]
    normed[:, width:] = jnp.zeros((rows, normed.shape[1] - width), F32)
    for d in range(dp):
        first = share * d
        low = first // LANES * LANES
        window = normed[:, low : low + share_pad + LANES]
        if first != low:
            window = pltpu.roll(window, window.shape[1] - (first - low), 1)
        slots[d] = window[:, :share_pad].astype(BF16)

    pl.semaphore_wait(barrier, dp - 1 + side * (tensor - 1))

    sends = []

    def send(src, dst, send_sem, recv_sem, device):
        copy = pltpu.make_async_remote_copy(
            src_ref=src, dst_ref=dst, send_sem=send_sem, recv_sem=recv_sem, device_id=device, device_id_type=MESH
        )
        copy.start()
        sends.append(copy)
        return copy

    first_copies = [None] * dp
    for k in range(1, dp):
        peer = plane_peer(plane[k])
        first_copies[k] = send(slots.at[peer], spread.at[k], s1.at[k], r1.at[k], {"dp": peer})
    spread[0] = slots[me]
    early = -(-share // 32) * 16
    ways = ((1, 0, early), (side - 1, share - early, 0))
    c_ow.wait()
    early_copies = []
    for way, (step, first, _) in enumerate(ways):
        piece = rows_of(my_y, first, early)
        early_copies.append(send(piece, piece, sw.at[way, 0], rw.at[way, 0], {"dp": plane_peer((0, step))}))

    c_k, c_v = [], []
    for b in range(rows):
        copy = pltpu.make_async_copy(kc_hbm.at[b], kcache.at[b], cache_sem.at[0, b])
        copy.start()
        c_k.append(copy)
    for b in range(rows):
        copy = pltpu.make_async_copy(vc_hbm.at[b], vcache.at[b], cache_sem.at[1, b])
        copy.start()
        c_v.append(copy)

    weights[share:, :] = jnp.zeros((share_pad - share, weights.shape[1]), BF16)
    for copy in c_small:
        copy.wait()
    sub = lax.broadcasted_iota(jnp.int32, (rows, rows), 0)
    lane = lax.broadcasted_iota(jnp.int32, (rows, rows), 1)
    pos_col = jnp.sum(jnp.where(sub == lane, positions[...].astype(F32), 0.0), axis=1, keepdims=True)
    angles = (pos_col * (1.0 / ROPE_FACTOR)) * freq[...]
    cos_part = jnp.cos(angles)
    half = lax.broadcasted_iota(jnp.int32, (rows, HD), 1) < HD // 2
    sin_part = jnp.where(half, -jnp.sin(angles), jnp.sin(angles))
    len_row = jnp.concatenate([lengths[...]] * heads + [jnp.zeros((1, HD // 2 - heads * rows), jnp.int32)] * (heads * rows < HD // 2), axis=1)
    len_row = jnp.concatenate([len_row, len_row], axis=1)
    own_rows = lax.broadcasted_iota(jnp.int32, (rows, LANES), 0)
    for tile in range(width // LANES):
        block = tokens[:, tile * LANES : (tile + 1) * LANES].astype(F32)
        for i in range(mine):
            tok_mine[i : i + 1, tile * LANES : (tile + 1) * LANES] = jnp.sum(
                jnp.where(own_rows == me_t * mine + i, block, 0.0), axis=0, keepdims=True
            )
    for copy in c_w:
        copy.wait()

    group = max(dp // 4, 1)
    own_part = None
    second_copies = [None] * dp
    for g0 in range(0, dp, group):
        for k in range(max(g0, 1), g0 + group):
            first_copies[k].wait_recv()
        lhs = spread[g0 : g0 + group].reshape(group * rows, share_pad)
        part = jnp.dot(lhs, weights[...], preferred_element_type=F32)
        if g0 == 0:
            own_part = part[:rows]
        part_out[g0 : g0 + group] = part.astype(BF16).reshape(group, rows, part.shape[1])
        for k in range(max(g0, 1), g0 + group):
            second_copies[k] = send(
                part_out.at[k], part_in.at[k], s2.at[k], r2.at[k], {"dp": plane_source(plane[k])}
            )

    joined = own_part
    for k in range(1, dp):
        second_copies[k].wait_recv()
        joined = joined + part_in[k].astype(F32)

    late_copies = []
    for copy in early_copies:
        copy.wait_recv()
    for way, (step, first, rest) in enumerate(ways):
        piece = rows_of(ys[-step], way * early, early if way == 0 else share - early)
        late_copies.append(send(piece, piece, sw.at[way, 1], rw.at[way, 1], {"dp": plane_peer((0, step))}))
        piece = rows_of(my_y, rest, share - early)
        late_copies.append(send(piece, piece, sw.at[way, 2], rw.at[way, 2], {"dp": plane_peer((0, step))}))

    def rms_rope(vectors, gain):
        square = jnp.sum(vectors * vectors, axis=1, keepdims=True) * (1.0 / HD)
        scaled = vectors * lax.rsqrt(square + EPS) * gain
        return scaled * cos_part + pltpu.roll(scaled, HD // 2, 1) * sin_part

    queries = [
        (rms_rope(joined[:, h * HD : (h + 1) * HD], q_gain[...]) * QPRE ** (-0.5)).astype(BF16) for h in range(heads)
    ]
    new_keys = jnp.concatenate(
        [rms_rope(joined[:, q_cols + g * HD : q_cols + (g + 1) * HD], k_gain[...]) for g in range(kv_heads)], axis=1
    ).astype(BF16)
    new_values = joined[:, q_cols + kv_cols :].astype(BF16)
    nk_out[...] = new_keys
    nv_out[...] = new_values

    zero_head = jnp.zeros((rows, HD), BF16)
    stacked = [
        jnp.concatenate([queries[h] if g == h // per_kv else zero_head for g in range(kv_heads)], axis=1)
        for h in range(heads)
    ]
    used = heads * rows
    if used < HD // 2:
        stacked.append(jnp.zeros((HD // 2 - used, kv_cols), BF16))
    query_rows = jnp.concatenate(stacked, axis=0)
    half_rows = HD // 2
    query_of = lax.broadcasted_iota(jnp.int32, (half_rows, 1), 0) % rows
    zeros_half = jnp.zeros((half_rows, kv_cols), BF16)
    picks = [(query_of == b).astype(F32).astype(BF16) for b in range(rows)]
    contract_last = (((1,), (1,)), ((), ()))
    for copy in c_k:
        copy.wait()
    slots_half = ctx // 2
    block_rows = min(256, slots_half)
    blocks = slots_half // block_rows
    low_q, high_q = [], []
    for b in range(rows):
        only = query_rows * picks[b]
        low_q.append(jnp.concatenate([only, zeros_half], axis=0))
        high_q.append(jnp.concatenate([zeros_half, only], axis=0))
    lane_row = lax.broadcasted_iota(jnp.int32, (1, HD), 1)
    base_slot = jnp.where(lane_row < half_rows, 0, slots_half)
    largest = None
    for m in range(blocks):
        total = None
        for b in range(rows):
            low = lax.dot_general(
                kcache[b, m * block_rows : (m + 1) * block_rows, :], low_q[b], contract_last, preferred_element_type=F32
            )
            high = lax.dot_general(
                kcache[b, slots_half + m * block_rows : slots_half + (m + 1) * block_rows, :], high_q[b],
                contract_last, preferred_element_type=F32,
            )
            total = low + high if total is None else total + low + high
        slot = lax.broadcasted_iota(jnp.int32, (block_rows, HD), 0) + (m * block_rows) + base_slot
        total = jnp.where(slot < len_row, total, -jnp.inf)
        scores[m * block_rows : (m + 1) * block_rows, :] = total
        top = jnp.max(total, axis=0, keepdims=True)
        largest = top if largest is None else jnp.maximum(largest, top)
    own_scores = lax.dot_general(
        new_keys, jnp.concatenate([query_rows, query_rows], axis=0), contract_last, preferred_element_type=F32
    )
    own_lane = lax.broadcasted_iota(jnp.int32, (rows, HD), 1) % rows
    own_diag = lax.broadcasted_iota(jnp.int32, (rows, HD), 0) == own_lane
    own_row = jnp.sum(jnp.where(own_diag, own_scores, 0.0), axis=0, keepdims=True)
    largest = jnp.maximum(jnp.maximum(largest, pltpu.roll(largest, half_rows, 1)), own_row)
    own_weight = jnp.exp(own_row - largest)
    total_row = None
    for m in range(blocks):
        weight = jnp.exp(scores[m * block_rows : (m + 1) * block_rows, :] - largest)
        part_total = jnp.sum(weight, axis=0, keepdims=True)
        total_row = part_total if total_row is None else total_row + part_total
        probs[:, m * block_rows : (m + 1) * block_rows] = weight.T.astype(BF16)
    total_row = total_row + pltpu.roll(total_row, half_rows, 1) + own_weight
    eye = lax.broadcasted_iota(jnp.int32, (half_rows, HD), 0) == lax.broadcasted_iota(jnp.int32, (half_rows, HD), 1)
    total_col = jnp.sum(jnp.where(eye, total_row, 0.0), axis=1, keepdims=True)
    own_mix = jnp.where(own_diag, own_weight, 0.0)[:, :half_rows].astype(BF16)
    mixture = lax.dot_general(own_mix, new_values, (((0,), (0,)), ((), ())), preferred_element_type=F32)
    for copy in c_v:
        copy.wait()
    low_p = probs[:half_rows, :]
    high_p = probs[half_rows:, :]
    for b in range(rows):
        mixture = mixture + jnp.dot(low_p * picks[b], vcache[b, :slots_half, :], preferred_element_type=F32)
        mixture = mixture + jnp.dot(high_p * picks[b], vcache[b, slots_half:, :], preferred_element_type=F32)
    mixture = mixture / total_col
    attended = jnp.concatenate(
        [mixture[h * rows : (h + 1) * rows, (h // per_kv) * HD : (h // per_kv + 1) * HD] for h in range(heads)], axis=1
    ).astype(BF16)

    att_in[0] = attended
    third_copies = [None] * side
    for k in reversed(range(1, side)):
        third_copies[k] = send(
            att_in.at[0], att_in.at[k], s3.at[k], r3.at[k], {"dp": plane_peer((ring[k], 0))}
        )
    for copy in late_copies:
        copy.wait_recv()
    for k in range(1, side):
        third_copies[k].wait_recv()
    products = lax.dot_general(
        att_in[...].reshape(side * rows, q_cols), oweight[...], contract_last, preferred_element_type=F32
    ).astype(BF16)

    for k in range(side):
        for t in range(tensor):
            first = k * rows + t * mine
            red_out[k, t] = products[first : first + mine, :]
    fourth_copies = []
    for k in reversed(range(side)):
        for step in reversed(range(tensor)):
            if k or step:
                peer_t = line_peer(line[step])
                fourth_copies.append(
                    send(
                        red_out.at[k, peer_t], red_in.at[my_x, step], s4.at[k, step], r4.at[k, step],
                        {"dp": plane_source((ring[k], 0)), "tensor": peer_t},
                    )
                )
    red_in[my_x, 0] = red_out[0, me_t]
    for copy in fourth_copies:
        copy.wait_recv()
    tiles = [jnp.zeros((mine, LANES), F32) for _ in range(width // LANES)]
    for column in range(side):
        low = column * side * share // LANES
        for c in range(strip // LANES):
            if low + c < len(tiles):
                for step in range(tensor):
                    tiles[low + c] = tiles[low + c] + red_in[column, step, :, c * LANES : (c + 1) * LANES].astype(F32)
    square = tiles[0] * tiles[0]
    for tile in tiles[1:]:
        square = square + tile * tile
    scale = lax.rsqrt(jnp.sum(square, axis=1, keepdims=True) * (1.0 / width) + EPS)
    projected = jnp.concatenate(tiles, axis=1)
    row_out[...] = (tok_mine[...] + projected * scale * post_gain[...]).astype(BF16)

    keep = pltpu.make_async_copy(row_out, hid_hbm.at[me_t], last_sem)
    keep.start()
    fifth_copies = [
        send(row_out, hid_hbm.at[me_t], s5.at[k], r5.at[k], {"tensor": line_peer(line[k])})
        for k in reversed(range(1, tensor))
    ]
    for copy in fifth_copies:
        copy.wait_recv()
    keep.wait()
    for copy in sends:
        copy.wait_send()


def finish_kernel(hid_in, nk_in, nv_in, hid, nk, nv):
    hid[...] = hid_in[...].reshape(hid.shape)
    nk[...] = nk_in[...]
    nv[...] = nv_in[...]


def per_device(dp, tensor, side, *args):
    tokens, lengths, positions, in_gain, qw, kw, vw, q_gain, k_gain, kc, vc, ow, post_gain = args
    rows, width = tokens.shape
    share, q_cols = qw.shape
    kv_cols = kw.shape[1]
    ctx = kc.shape[1]
    share_pad = padded(share)
    cols = q_cols + 2 * kv_cols
    mine = rows // tensor
    strip = padded(side * share + max(side * share * a % LANES for a in range(side)))
    dims = (dp, tensor, side, rows, width, share, q_cols, kv_cols, ctx, strip)
    exponent = np.arange(HD // 2, dtype=np.float64) * (2.0 / HD)
    frequency = (ROPE_BASE**-exponent).astype(np.float32)
    freq = jnp.asarray(np.concatenate([frequency, frequency])[None])
    any_spec = pl.BlockSpec(memory_space=pl.ANY)
    vmem_spec = pl.BlockSpec(memory_space=pltpu.VMEM)
    dma = pltpu.SemaphoreType.DMA
    hidden, new_keys, new_values = pl.pallas_call(
        functools.partial(kernel, dims),
        out_shape=(
            jax.ShapeDtypeStruct((tensor, mine, width), BF16),
            jax.ShapeDtypeStruct((rows, kv_cols), BF16),
            jax.ShapeDtypeStruct((rows, kv_cols), BF16),
        ),
        in_specs=[any_spec] * 14,
        out_specs=(any_spec, vmem_spec, vmem_spec),
        scratch_shapes=[
            pltpu.VMEM((rows, width), BF16),
            pltpu.VMEM((1, rows), jnp.int32),
            pltpu.VMEM((1, rows), jnp.int32),
            pltpu.VMEM((1, width), F32),
            pltpu.VMEM((share_pad, cols), BF16),
            pltpu.VMEM((1, HD), F32),
            pltpu.VMEM((1, HD), F32),
            pltpu.VMEM((rows, ctx, kv_cols), BF16),
            pltpu.VMEM((rows, ctx, kv_cols), BF16),
            pltpu.VMEM((strip, q_cols), BF16),
            pltpu.VMEM((1, width), F32),
            pltpu.VMEM((1, HD), F32),
            pltpu.VMEM((rows, width + 2 * LANES), F32),
            pltpu.VMEM((mine, width), F32),
            pltpu.VMEM((dp, rows, share_pad), BF16),
            pltpu.VMEM((dp, rows, share_pad), BF16),
            pltpu.VMEM((dp, rows, cols), BF16),
            pltpu.VMEM((dp, rows, cols), BF16),
            pltpu.VMEM((ctx // 2, HD), F32),
            pltpu.VMEM((HD, ctx // 2), BF16),
            pltpu.VMEM((side, rows, q_cols), BF16),
            pltpu.VMEM((side, tensor, mine, strip), BF16),
            pltpu.VMEM((side, tensor, mine, strip), BF16),
            pltpu.VMEM((mine, width), BF16),
            dma((12,)),
            dma((2, rows)),
            dma((dp,)), dma((dp,)),
            dma((dp,)), dma((dp,)),
            dma((side,)), dma((side,)),
            dma((side, tensor)), dma((side, tensor)),
            dma((tensor,)), dma((tensor,)),
            dma((2, 3)), dma((2, 3)),
            dma(()),
        ],
        compiler_params=pltpu.CompilerParams(collective_id=0, has_side_effects=True, vmem_limit_bytes=50 * 1024 * 1024),
    )(
        *[
            pltpu.with_memory_space_constraint(operand, pltpu.HBM)
            for operand in (
                tokens, lengths.reshape(1, rows), positions.reshape(1, rows), in_gain, qw, kw, vw,
                q_gain.reshape(1, HD), k_gain.reshape(1, HD), kc, vc, ow.T, post_gain, freq,
            )
        ]
    )
    return pl.pallas_call(
        finish_kernel,
        out_shape=(
            jax.ShapeDtypeStruct((rows, width), BF16),
            jax.ShapeDtypeStruct((rows, kv_cols), BF16),
            jax.ShapeDtypeStruct((rows, kv_cols), BF16),
        ),
        compiler_params=pltpu.CompilerParams(vmem_limit_bytes=4 * 1024 * 1024),
    )(hidden, new_keys, new_values)


def solution(mesh):
    dp, tensor = mesh.shape["dp"], mesh.shape["tensor"]
    side = int(round(dp**0.5))
    return jax.shard_map(
        functools.partial(per_device, dp, tensor, side),
        mesh=mesh,
        in_specs=(
            P("dp", None), P("dp"), P("dp"), P(), P("dp", "tensor"), P("dp", "tensor"), P("dp", "tensor"), P(), P(),
            P("dp", None, "tensor"), P("dp", None, "tensor"), P("tensor", "dp"), P(),
        ),
        out_specs=(P("dp", None), P("dp", "tensor"), P("dp", "tensor")),
        check_vma=False,
    )
```

```python
import functools

import jax
import jax.numpy as jnp
import numpy as np
from jax import lax
from jax.experimental import pallas as pl
from jax.experimental.pallas import tpu as pltpu
from jax.sharding import PartitionSpec as P

HD = 128
QPRE = 168
LANES = 128
EPS = 1e-06
ROPE_BASE = 1000000.0
ROPE_FACTOR = 8.0
MESH = pl.DeviceIdType.MESH
F32 = jnp.float32
BF16 = jnp.bfloat16


def padded(width):
    return -(-width // LANES) * LANES


def ring_distance(step, size):
    return min(step % size, -step % size)


def plane_offsets(side):
    steps = [(a, b) for a in range(side) for b in range(side)]
    return sorted(steps, key=lambda s: (ring_distance(s[0], side) + ring_distance(s[1], side), s))


def line_offsets(depth):
    steps = [(a, c) for a in range(depth) for c in range(2)]
    return sorted(steps, key=lambda s: (ring_distance(s[0], depth), s[1]))


def kernel(
    dims,
    tokens_hbm, lengths_hbm, positions_hbm, in_gain_hbm, qw_hbm, kw_hbm, vw_hbm, q_gain_hbm, k_gain_hbm,
    kc_hbm, vc_hbm, ow_hbm, post_gain_hbm, freq_hbm,
    hid_hbm, nk_out, nv_out,
    tokens, lengths, positions, in_gain, weights, q_gain, k_gain, kcache, vcache, oweight, post_gain, freq,
    normed, tok_mine, slots, spread, part_out, part_in, other_out, other_in, scores, probs, att_in, red_out, red_in, row_out,
    load_sem, cache_sem, s1, r1, s2, r2, s3, r3, s4, r4, s5, r5, sw, rw, last_sem,
):
    dp, tensor, side, rows, width, share, q_cols, kv_cols, ctx, strip = dims
    depth = tensor // 2
    mine = rows // tensor
    heads = q_cols // HD
    kv_heads = kv_cols // HD
    per_kv = heads // kv_heads
    share_pad = padded(share)
    me = lax.axis_index("dp")
    me_t = lax.axis_index("tensor")
    my_x, my_y = lax.div(me, side), lax.rem(me, side)
    my_z, my_c = lax.div(me_t, 2), lax.rem(me_t, 2)
    xs = [my_x] + [lax.rem(my_x + a, side) for a in range(1, side)]
    ys = [my_y] + [lax.rem(my_y + a, side) for a in range(1, side)]
    zs = [my_z] + [lax.rem(my_z + a, depth) for a in range(1, depth)]
    cs = [my_c, 1 - my_c]

    def plane_peer(step):
        return xs[step[0]] * side + ys[step[1]]

    def plane_source(step):
        return xs[-step[0]] * side + ys[-step[1]]

    first_core = my_c == 0
    place = jnp.where(first_core, my_x, my_y)
    across = jnp.where(first_core, my_y, my_x)
    along_x = [xs[a] * side + my_y for a in range(side)]
    along_y = [my_x * side + ys[a] for a in range(side)]

    def gather_peer(a):
        return jnp.where(first_core, along_y[a], along_x[a])

    def spread_peer(a):
        return jnp.where(first_core, along_x[a], along_y[a])

    def line_peer(step):
        return zs[step[0]] * 2 + cs[step[1]]

    plane = plane_offsets(side)
    line = line_offsets(depth)
    ring = sorted(range(side), key=lambda a: (ring_distance(a, side), a))

    for a in range(side):
        oweight[a * share_pad + share : (a + 1) * share_pad, :] = jnp.zeros((share_pad - share, q_cols), BF16)

    barrier = pltpu.get_barrier_semaphore()
    greeted = [({"dp": plane_peer(step)}) for step in reversed(plane[1:])]
    for step in reversed(line[1:]):
        greeted.append({"tensor": line_peer(step)})
        for a in range(1, side):
            if step[1]:
                greeted.append({"dp": along_x[a], "tensor": line_peer(step)})
                greeted.append({"dp": along_y[a], "tensor": line_peer(step)})
            else:
                greeted.append({"dp": spread_peer(a), "tensor": line_peer(step)})
    for device in greeted:
        pl.semaphore_signal(barrier, inc=1, device_id=device, device_id_type=MESH)

    def load(src, dst, at):
        copy = pltpu.make_async_copy(src, dst, load_sem.at[at])
        copy.start()
        return copy

    c_tokens = load(tokens_hbm, tokens, 0)
    c_gain = load(in_gain_hbm, in_gain.at[0], 1)
    c_w = [
        load(qw_hbm, weights.at[pl.ds(0, share), pl.ds(0, q_cols)], 2),
        load(kw_hbm, weights.at[pl.ds(0, share), pl.ds(q_cols, kv_cols)], 3),
        load(vw_hbm, weights.at[pl.ds(0, share), pl.ds(q_cols + kv_cols, kv_cols)], 4),
    ]
    c_small = [
        load(lengths_hbm, lengths, 5), load(positions_hbm, positions, 6), load(q_gain_hbm, q_gain, 7),
        load(k_gain_hbm, k_gain, 8), load(post_gain_hbm, post_gain.at[0], 9), load(freq_hbm, freq, 10),
    ]
    def rows_of(at, first, count):
        return oweight.at[pl.ds(pl.multiple_of(at * share_pad + first, 16), count), :]

    own_block = rows_of(across, 0, share)
    c_ow = load(ow_hbm, own_block, 11)

    c_tokens.wait()
    c_gain.wait()
    x = tokens[...].astype(F32)
    mean_square = jnp.sum(x * x, axis=1, keepdims=True) * (1.0 / width)
    normed[:, :width] = x * lax.rsqrt(mean_square + EPS) * in_gain[...]
    normed[:, width:] = jnp.zeros((rows, normed.shape[1] - width), F32)
    for d in range(dp):
        first = share * d
        low = first // LANES * LANES
        window = normed[:, low : low + share_pad + LANES]
        if first != low:
            window = pltpu.roll(window, window.shape[1] - (first - low), 1)
        slots[d] = window[:, :share_pad].astype(BF16)

    pl.semaphore_wait(barrier, len(greeted))

    sends = []

    def send(src, dst, send_sem, recv_sem, device):
        copy = pltpu.make_async_remote_copy(
            src_ref=src, dst_ref=dst, send_sem=send_sem, recv_sem=recv_sem, device_id=device, device_id_type=MESH
        )
        copy.start()
        sends.append(copy)
        return copy

    first_copies = [None] * dp
    for k in range(1, dp):
        peer = plane_peer(plane[k])
        first_copies[k] = send(slots.at[peer], spread.at[k], s1.at[k], r1.at[k], {"dp": peer})
    spread[0] = slots[me]
    far = -(-share // 32) * 16
    c_ow.wait()
    ways = ((1, 0, far), (side - 1, far, share - far))
    early_copies = []
    for way, (step, first, count) in enumerate(ways):
        piece = rows_of(across, first, count)
        early_copies.append(send(piece, piece, sw.at[way, 0], rw.at[way, 0], {"dp": gather_peer(step)}))

    c_k, c_v = [], []
    for b in range(rows):
        copy = pltpu.make_async_copy(kc_hbm.at[b], kcache.at[b], cache_sem.at[0, b])
        copy.start()
        c_k.append(copy)
    for b in range(rows):
        copy = pltpu.make_async_copy(vc_hbm.at[b], vcache.at[b], cache_sem.at[1, b])
        copy.start()
        c_v.append(copy)

    weights[share:, :] = jnp.zeros((share_pad - share, weights.shape[1]), BF16)
    for copy in c_small:
        copy.wait()
    sub = lax.broadcasted_iota(jnp.int32, (rows, rows), 0)
    lane = lax.broadcasted_iota(jnp.int32, (rows, rows), 1)
    pos_col = jnp.sum(jnp.where(sub == lane, positions[...].astype(F32), 0.0), axis=1, keepdims=True)
    angles = (pos_col * (1.0 / ROPE_FACTOR)) * freq[...]
    cos_part = jnp.cos(angles)
    half = lax.broadcasted_iota(jnp.int32, (rows, HD), 1) < HD // 2
    sin_part = jnp.where(half, -jnp.sin(angles), jnp.sin(angles))
    len_row = jnp.concatenate([lengths[...]] * heads + [jnp.zeros((1, HD // 2 - heads * rows), jnp.int32)] * (heads * rows < HD // 2), axis=1)
    len_row = jnp.concatenate([len_row, len_row], axis=1)
    own_rows = lax.broadcasted_iota(jnp.int32, (rows, LANES), 0)
    for tile in range(width // LANES):
        block = tokens[:, tile * LANES : (tile + 1) * LANES].astype(F32)
        for i in range(mine):
            tok_mine[i : i + 1, tile * LANES : (tile + 1) * LANES] = jnp.sum(
                jnp.where(own_rows == me_t * mine + i, block, 0.0), axis=0, keepdims=True
            )
    for copy in c_w:
        copy.wait()

    group = max(dp // 4, 1)
    own_part = None
    second_copies, other_copies = [None] * dp, [None] * dp
    for g0 in range(0, dp, group):
        for k in range(max(g0, 1), g0 + group):
            first_copies[k].wait_recv()
        lhs = spread[g0 : g0 + group].reshape(group * rows, share_pad)
        part = jnp.dot(lhs, weights[...], preferred_element_type=F32)
        if g0 == 0:
            own_part = part[:rows]
        sent = part.astype(BF16).reshape(group, rows, part.shape[1])
        part_out[g0 : g0 + group] = sent[:, :, :q_cols]
        other_out[g0 : g0 + group] = sent[:, :, q_cols:]
        for k in range(max(g0, 1), g0 + group):
            second_copies[k] = send(
                part_out.at[k], part_in.at[k], s2.at[0, k], r2.at[0, k], {"dp": plane_source(plane[k])}
            )
    for k in range(1, dp):
        other_copies[k] = send(
            other_out.at[k], other_in.at[k], s2.at[1, k], r2.at[1, k], {"dp": plane_source(plane[k])}
        )

    joined = own_part[:, :q_cols]
    for k in range(1, dp):
        second_copies[k].wait_recv()
        joined = joined + part_in[k].astype(F32)

    for copy in early_copies:
        copy.wait_recv()
    late_copies = []
    for way, (step, first, count) in enumerate(ways):
        piece = rows_of(jnp.where(first_core, ys[-step], xs[-step]), first, count)
        late_copies.append(send(piece, piece, sw.at[way, 1], rw.at[way, 1], {"dp": gather_peer(step)}))
        piece = rows_of(across, *ways[1 - way][1:])
        late_copies.append(send(piece, piece, sw.at[way, 2], rw.at[way, 2], {"dp": gather_peer(step)}))

    def rms_rope(vectors, gain):
        square = jnp.sum(vectors * vectors, axis=1, keepdims=True) * (1.0 / HD)
        scaled = vectors * lax.rsqrt(square + EPS) * gain
        return scaled * cos_part + pltpu.roll(scaled, HD // 2, 1) * sin_part

    queries = [
        (rms_rope(joined[:, h * HD : (h + 1) * HD], q_gain[...]) * QPRE ** (-0.5)).astype(BF16) for h in range(heads)
    ]
    zero_head = jnp.zeros((rows, HD), BF16)
    stacked = [
        jnp.concatenate([queries[h] if g == h // per_kv else zero_head for g in range(kv_heads)], axis=1)
        for h in range(heads)
    ]
    used = heads * rows
    if used < HD // 2:
        stacked.append(jnp.zeros((HD // 2 - used, kv_cols), BF16))
    query_rows = jnp.concatenate(stacked, axis=0)
    half_rows = HD // 2
    query_of = lax.broadcasted_iota(jnp.int32, (half_rows, 1), 0) % rows
    zeros_half = jnp.zeros((half_rows, kv_cols), BF16)
    picks = [(query_of == b).astype(F32).astype(BF16) for b in range(rows)]
    contract_last = (((1,), (1,)), ((), ()))
    for copy in c_k:
        copy.wait()
    slots_half = ctx // 2
    block_rows = min(256, slots_half)
    blocks = slots_half // block_rows
    low_q, high_q = [], []
    for b in range(rows):
        only = query_rows * picks[b]
        low_q.append(jnp.concatenate([only, zeros_half], axis=0))
        high_q.append(jnp.concatenate([zeros_half, only], axis=0))
    lane_row = lax.broadcasted_iota(jnp.int32, (1, HD), 1)
    base_slot = jnp.where(lane_row < half_rows, 0, slots_half)
    largest = None
    for m in range(blocks):
        total = None
        for b in range(rows):
            low = lax.dot_general(
                kcache[b, m * block_rows : (m + 1) * block_rows, :], low_q[b], contract_last, preferred_element_type=F32
            )
            high = lax.dot_general(
                kcache[b, slots_half + m * block_rows : slots_half + (m + 1) * block_rows, :], high_q[b],
                contract_last, preferred_element_type=F32,
            )
            total = low + high if total is None else total + low + high
        slot = lax.broadcasted_iota(jnp.int32, (block_rows, HD), 0) + (m * block_rows) + base_slot
        total = jnp.where(slot < len_row, total, -jnp.inf)
        scores[m * block_rows : (m + 1) * block_rows, :] = total
        top = jnp.max(total, axis=0, keepdims=True)
        largest = top if largest is None else jnp.maximum(largest, top)
    others = own_part[:, q_cols:]
    for k in range(1, dp):
        other_copies[k].wait_recv()
        others = others + other_in[k].astype(F32)
    new_keys = jnp.concatenate(
        [rms_rope(others[:, g * HD : (g + 1) * HD], k_gain[...]) for g in range(kv_heads)], axis=1
    ).astype(BF16)
    new_values = others[:, kv_cols:].astype(BF16)
    nk_out[...] = new_keys
    nv_out[...] = new_values

    own_scores = lax.dot_general(
        new_keys, jnp.concatenate([query_rows, query_rows], axis=0), contract_last, preferred_element_type=F32
    )
    own_lane = lax.broadcasted_iota(jnp.int32, (rows, HD), 1) % rows
    own_diag = lax.broadcasted_iota(jnp.int32, (rows, HD), 0) == own_lane
    own_row = jnp.sum(jnp.where(own_diag, own_scores, 0.0), axis=0, keepdims=True)
    largest = jnp.maximum(jnp.maximum(largest, pltpu.roll(largest, half_rows, 1)), own_row)
    own_weight = jnp.exp(own_row - largest)
    total_row = None
    for m in range(blocks):
        weight = jnp.exp(scores[m * block_rows : (m + 1) * block_rows, :] - largest)
        part_total = jnp.sum(weight, axis=0, keepdims=True)
        total_row = part_total if total_row is None else total_row + part_total
        probs[:, m * block_rows : (m + 1) * block_rows] = weight.T.astype(BF16)
    total_row = total_row + pltpu.roll(total_row, half_rows, 1) + own_weight
    eye = lax.broadcasted_iota(jnp.int32, (half_rows, HD), 0) == lax.broadcasted_iota(jnp.int32, (half_rows, HD), 1)
    total_col = jnp.sum(jnp.where(eye, total_row, 0.0), axis=1, keepdims=True)
    own_mix = jnp.where(own_diag, own_weight, 0.0)[:, :half_rows].astype(BF16)
    mixture = lax.dot_general(own_mix, new_values, (((0,), (0,)), ((), ())), preferred_element_type=F32)
    for copy in c_v:
        copy.wait()
    low_p = probs[:half_rows, :]
    high_p = probs[half_rows:, :]
    for b in range(rows):
        mixture = mixture + jnp.dot(low_p * picks[b], vcache[b, :slots_half, :], preferred_element_type=F32)
        mixture = mixture + jnp.dot(high_p * picks[b], vcache[b, slots_half:, :], preferred_element_type=F32)
    mixture = mixture / total_col
    attended = jnp.concatenate(
        [mixture[h * rows : (h + 1) * rows, (h // per_kv) * HD : (h // per_kv + 1) * HD] for h in range(heads)], axis=1
    ).astype(BF16)

    att_in[0] = attended
    third_copies = [None] * side
    for k in reversed(range(1, side)):
        third_copies[k] = send(
            att_in.at[0], att_in.at[k], s3.at[k], r3.at[k], {"dp": spread_peer(ring[k])}
        )
    for copy in late_copies:
        copy.wait_recv()
    for k in range(1, side):
        third_copies[k].wait_recv()
    products = lax.dot_general(
        att_in[...].reshape(side * rows, q_cols), oweight[...], contract_last, preferred_element_type=F32
    ).astype(BF16)

    for k in range(side):
        for t in range(tensor):
            first = k * rows + t * mine
            red_out[k, t] = products[first : first + mine, :]
    fourth_copies = []
    for k in reversed(range(side)):
        for turn, (step_z, step_c) in reversed(list(enumerate(line))):
            if k or turn:
                peer_t = line_peer((step_z, step_c))
                slot = red_in.at[my_c, place, step_z]
                fourth_copies.append(
                    send(
                        red_out.at[k, peer_t], slot, s4.at[k, turn], r4.at[k, turn],
                        {"dp": spread_peer(-ring[k] % side), "tensor": peer_t},
                    )
                )
    red_in[my_c, place, 0] = red_out[0, me_t]
    for copy in fourth_copies:
        copy.wait_recv()
    tiles = [jnp.zeros((mine, LANES), F32) for _ in range(width // LANES)]
    lane_pair = lax.broadcasted_iota(jnp.int32, (mine, LANES), 1)
    for d in range(dp):
        parts = []
        for c, p, a in ((0, d // side, d % side), (1, d % side, d // side)):
            for z in range(depth):
                parts.append(red_in[c, p, z, :, a * share_pad : (a + 1) * share_pad].astype(F32))
        while len(parts) > 1:
            parts = [parts[n] + parts[n + 1] for n in range(0, len(parts) - 1, 2)] + parts[len(parts) // 2 * 2 :]
        low, turn = share * d // LANES, share * d % LANES
        columns = [parts[0][:, n * LANES : (n + 1) * LANES] for n in range(share_pad // LANES)]
        if turn:
            columns = [pltpu.roll(column, turn, 1) for column in columns]
            none = jnp.zeros((mine, LANES), F32)
            columns = [
                jnp.where(lane_pair < turn, before, after)
                for before, after in zip([none] + columns, columns + [none])
            ]
        for n, column in enumerate(columns):
            if low + n < len(tiles) and n * LANES < turn + share:
                tiles[low + n] = tiles[low + n] + column
    square = tiles[0] * tiles[0]
    for tile in tiles[1:]:
        square = square + tile * tile
    scale = lax.rsqrt(jnp.sum(square, axis=1, keepdims=True) * (1.0 / width) + EPS)
    projected = jnp.concatenate(tiles, axis=1)
    row_out[...] = (tok_mine[...] + projected * scale * post_gain[...]).astype(BF16)

    keep = pltpu.make_async_copy(row_out, hid_hbm.at[me_t], last_sem)
    keep.start()
    fifth_copies = [
        send(row_out, hid_hbm.at[me_t], s5.at[k], r5.at[k], {"tensor": line_peer(line[k])})
        for k in reversed(range(1, tensor))
    ]
    for copy in sends:
        copy.wait_send()
    keep.wait()
    for copy in fifth_copies:
        copy.wait_recv()


def finish_kernel(hid_in, nk_in, nv_in, hid, nk, nv):
    hid[...] = hid_in[...].reshape(hid.shape)
    nk[...] = nk_in[...]
    nv[...] = nv_in[...]


def per_device(dp, tensor, side, *args):
    tokens, lengths, positions, in_gain, qw, kw, vw, q_gain, k_gain, kc, vc, ow, post_gain = args
    rows, width = tokens.shape
    share, q_cols = qw.shape
    kv_cols = kw.shape[1]
    ctx = kc.shape[1]
    share_pad = padded(share)
    cols = q_cols + 2 * kv_cols
    mine = rows // tensor
    depth = tensor // 2
    strip = side * share_pad
    dims = (dp, tensor, side, rows, width, share, q_cols, kv_cols, ctx, strip)
    exponent = np.arange(HD // 2, dtype=np.float64) * (2.0 / HD)
    frequency = (ROPE_BASE**-exponent).astype(np.float32)
    freq = jnp.asarray(np.concatenate([frequency, frequency])[None])
    any_spec = pl.BlockSpec(memory_space=pl.ANY)
    vmem_spec = pl.BlockSpec(memory_space=pltpu.VMEM)
    dma = pltpu.SemaphoreType.DMA
    hidden, new_keys, new_values = pl.pallas_call(
        functools.partial(kernel, dims),
        out_shape=(
            jax.ShapeDtypeStruct((tensor, mine, width), BF16),
            jax.ShapeDtypeStruct((rows, kv_cols), BF16),
            jax.ShapeDtypeStruct((rows, kv_cols), BF16),
        ),
        in_specs=[any_spec] * 14,
        out_specs=(any_spec, vmem_spec, vmem_spec),
        scratch_shapes=[
            pltpu.VMEM((rows, width), BF16),
            pltpu.VMEM((1, rows), jnp.int32),
            pltpu.VMEM((1, rows), jnp.int32),
            pltpu.VMEM((1, width), F32),
            pltpu.VMEM((share_pad, cols), BF16),
            pltpu.VMEM((1, HD), F32),
            pltpu.VMEM((1, HD), F32),
            pltpu.VMEM((rows, ctx, kv_cols), BF16),
            pltpu.VMEM((rows, ctx, kv_cols), BF16),
            pltpu.VMEM((strip, q_cols), BF16),
            pltpu.VMEM((1, width), F32),
            pltpu.VMEM((1, HD), F32),
            pltpu.VMEM((rows, width + 2 * LANES), F32),
            pltpu.VMEM((mine, width), F32),
            pltpu.VMEM((dp, rows, share_pad), BF16),
            pltpu.VMEM((dp, rows, share_pad), BF16),
            pltpu.VMEM((dp, rows, q_cols), BF16),
            pltpu.VMEM((dp, rows, q_cols), BF16),
            pltpu.VMEM((dp, rows, 2 * kv_cols), BF16),
            pltpu.VMEM((dp, rows, 2 * kv_cols), BF16),
            pltpu.VMEM((ctx // 2, HD), F32),
            pltpu.VMEM((HD, ctx // 2), BF16),
            pltpu.VMEM((side, rows, q_cols), BF16),
            pltpu.VMEM((side, tensor, mine, strip), BF16),
            pltpu.VMEM((2, side, depth, mine, strip), BF16),
            pltpu.VMEM((mine, width), BF16),
            dma((12,)),
            dma((2, rows)),
            dma((dp,)), dma((dp,)),
            dma((2, dp)), dma((2, dp)),
            dma((side,)), dma((side,)),
            dma((side, tensor)), dma((side, tensor)),
            dma((tensor,)), dma((tensor,)),
            dma((2, 3)), dma((2, 3)),
            dma(()),
        ],
        compiler_params=pltpu.CompilerParams(collective_id=0, has_side_effects=True, vmem_limit_bytes=50 * 1024 * 1024),
    )(
        *[
            pltpu.with_memory_space_constraint(operand, pltpu.HBM)
            for operand in (
                tokens, lengths.reshape(1, rows), positions.reshape(1, rows), in_gain, qw, kw, vw,
                q_gain.reshape(1, HD), k_gain.reshape(1, HD), kc, vc, ow.T, post_gain, freq,
            )
        ]
    )
    return pl.pallas_call(
        finish_kernel,
        out_shape=(
            jax.ShapeDtypeStruct((rows, width), BF16),
            jax.ShapeDtypeStruct((rows, kv_cols), BF16),
            jax.ShapeDtypeStruct((rows, kv_cols), BF16),
        ),
        compiler_params=pltpu.CompilerParams(vmem_limit_bytes=4 * 1024 * 1024),
    )(hidden, new_keys, new_values)


def solution(mesh):
    dp, tensor = mesh.shape["dp"], mesh.shape["tensor"]
    side = int(round(dp**0.5))
    return jax.shard_map(
        functools.partial(per_device, dp, tensor, side),
        mesh=mesh,
        in_specs=(
            P("dp", None), P("dp"), P("dp"), P(), P("dp", "tensor"), P("dp", "tensor"), P("dp", "tensor"), P(), P(),
            P("dp", None, "tensor"), P("dp", None, "tensor"), P("tensor", "dp"), P(),
        ),
        out_specs=(P("dp", None), P("dp", "tensor"), P("dp", "tensor")),
        check_vma=False,
    )
```

```python
import functools

import jax
import jax.numpy as jnp
import numpy as np
from jax import lax
from jax.experimental import pallas as pl
from jax.experimental.pallas import tpu as pltpu
from jax.sharding import PartitionSpec as P

HD = 128
QPRE = 168
LANES = 128
EPS = 1e-06
ROPE_BASE = 1000000.0
ROPE_FACTOR = 8.0
MESH = pl.DeviceIdType.MESH
F32 = jnp.float32
BF16 = jnp.bfloat16


def padded(width):
    return -(-width // LANES) * LANES


def ring_distance(step, size):
    return min(step % size, -step % size)


def plane_offsets(side):
    steps = [(a, b) for a in range(side) for b in range(side)]
    return sorted(steps, key=lambda s: (ring_distance(s[0], side) + ring_distance(s[1], side), s))


def line_offsets(depth):
    steps = [(a, c) for a in range(depth) for c in range(2)]
    return sorted(steps, key=lambda s: (ring_distance(s[0], depth), s[1]))


def kernel(
    dims,
    tokens_hbm, lengths_hbm, positions_hbm, in_gain_hbm, qw_hbm, kw_hbm, vw_hbm, q_gain_hbm, k_gain_hbm,
    kc_hbm, vc_hbm, ow_hbm, post_gain_hbm, freq_hbm,
    hid_hbm, nk_out, nv_out,
    tokens, lengths, positions, in_gain, weights, q_gain, k_gain, kcache, vcache, oweight, post_gain, freq,
    normed, tok_mine, slots, spread, part_out, part_in, other_out, other_in, scores, probs, att_in, red_out, red_in, row_out,
    load_sem, cache_sem, s1, r1, s2, r2, s3, r3, s4, r4, s5, r5, sw, rw, last_sem,
):
    dp, tensor, side, rows, width, share, q_cols, kv_cols, ctx, strip = dims
    depth = tensor // 2
    mine = rows // tensor
    heads = q_cols // HD
    kv_heads = kv_cols // HD
    per_kv = heads // kv_heads
    share_pad = padded(share)
    me = lax.axis_index("dp")
    me_t = lax.axis_index("tensor")
    my_x, my_y = lax.div(me, side), lax.rem(me, side)
    my_z, my_c = lax.div(me_t, 2), lax.rem(me_t, 2)
    xs = [my_x] + [lax.rem(my_x + a, side) for a in range(1, side)]
    ys = [my_y] + [lax.rem(my_y + a, side) for a in range(1, side)]
    zs = [my_z] + [lax.rem(my_z + a, depth) for a in range(1, depth)]
    cs = [my_c, 1 - my_c]

    def plane_peer(step):
        return xs[step[0]] * side + ys[step[1]]

    def plane_source(step):
        return xs[-step[0]] * side + ys[-step[1]]

    first_core = my_c == 0
    place = jnp.where(first_core, my_x, my_y)
    across = jnp.where(first_core, my_y, my_x)
    along_x = [xs[a] * side + my_y for a in range(side)]
    along_y = [my_x * side + ys[a] for a in range(side)]

    def gather_peer(a):
        return jnp.where(first_core, along_y[a], along_x[a])

    def spread_peer(a):
        return jnp.where(first_core, along_x[a], along_y[a])

    def line_peer(step):
        return zs[step[0]] * 2 + cs[step[1]]

    plane = plane_offsets(side)
    line = line_offsets(depth)
    ring = sorted(range(side), key=lambda a: (ring_distance(a, side), a))

    for a in range(side):
        oweight[a * share_pad + share : (a + 1) * share_pad, :] = jnp.zeros((share_pad - share, q_cols), BF16)

    barrier = pltpu.get_barrier_semaphore()
    greeted = [({"dp": plane_peer(step)}) for step in reversed(plane[1:])]
    for step in reversed(line[1:]):
        greeted.append({"tensor": line_peer(step)})
        for a in range(1, side):
            if step[1]:
                greeted.append({"dp": along_x[a], "tensor": line_peer(step)})
                greeted.append({"dp": along_y[a], "tensor": line_peer(step)})
            else:
                greeted.append({"dp": spread_peer(a), "tensor": line_peer(step)})
    for device in greeted:
        pl.semaphore_signal(barrier, inc=1, device_id=device, device_id_type=MESH)

    def load(src, dst, at):
        copy = pltpu.make_async_copy(src, dst, load_sem.at[at])
        copy.start()
        return copy

    c_tokens = load(tokens_hbm, tokens, 0)
    c_gain = load(in_gain_hbm, in_gain.at[0], 1)
    c_w = [
        load(qw_hbm, weights.at[pl.ds(0, share), pl.ds(0, q_cols)], 2),
        load(kw_hbm, weights.at[pl.ds(0, share), pl.ds(q_cols, kv_cols)], 3),
        load(vw_hbm, weights.at[pl.ds(0, share), pl.ds(q_cols + kv_cols, kv_cols)], 4),
    ]
    c_small = [
        load(lengths_hbm, lengths, 5), load(positions_hbm, positions, 6), load(q_gain_hbm, q_gain, 7),
        load(k_gain_hbm, k_gain, 8), load(post_gain_hbm, post_gain.at[0], 9), load(freq_hbm, freq, 10),
    ]
    def rows_of(at, first, count):
        return oweight.at[pl.ds(pl.multiple_of(at * share_pad + first, 16), count), :]

    own_block = rows_of(across, 0, share)
    c_ow = load(ow_hbm, own_block, 11)

    c_tokens.wait()
    c_gain.wait()
    x = tokens[...].astype(F32)
    mean_square = jnp.sum(x * x, axis=1, keepdims=True) * (1.0 / width)
    normed[:, :width] = x * lax.rsqrt(mean_square + EPS) * in_gain[...]
    normed[:, width:] = jnp.zeros((rows, normed.shape[1] - width), F32)
    for d in range(dp):
        first = share * d
        low = first // LANES * LANES
        window = normed[:, low : low + share_pad + LANES]
        if first != low:
            window = pltpu.roll(window, window.shape[1] - (first - low), 1)
        slots[d] = window[:, :share_pad].astype(BF16)

    pl.semaphore_wait(barrier, len(greeted))

    sends = []

    def send(src, dst, send_sem, recv_sem, device):
        copy = pltpu.make_async_remote_copy(
            src_ref=src, dst_ref=dst, send_sem=send_sem, recv_sem=recv_sem, device_id=device, device_id_type=MESH
        )
        copy.start()
        sends.append(copy)
        return copy

    first_copies = [None] * dp
    for k in reversed(range(1, dp)):
        peer = plane_peer(plane[k])
        first_copies[k] = send(slots.at[peer], spread.at[k], s1.at[k], r1.at[k], {"dp": peer})
    spread[0] = slots[me]
    far = -(-share // 32) * 16
    c_ow.wait()
    ways = ((1, 0, far), (side - 1, far, share - far))
    early_copies = []
    for way, (step, first, count) in enumerate(ways):
        piece = rows_of(across, first, count)
        early_copies.append(send(piece, piece, sw.at[way, 0], rw.at[way, 0], {"dp": gather_peer(step)}))

    c_k, c_v = [], []
    for b in range(rows):
        copy = pltpu.make_async_copy(kc_hbm.at[b], kcache.at[b], cache_sem.at[0, b])
        copy.start()
        c_k.append(copy)
    for b in range(rows):
        copy = pltpu.make_async_copy(vc_hbm.at[b], vcache.at[b], cache_sem.at[1, b])
        copy.start()
        c_v.append(copy)

    weights[share:, :] = jnp.zeros((share_pad - share, weights.shape[1]), BF16)
    for copy in c_small:
        copy.wait()
    sub = lax.broadcasted_iota(jnp.int32, (rows, rows), 0)
    lane = lax.broadcasted_iota(jnp.int32, (rows, rows), 1)
    pos_col = jnp.sum(jnp.where(sub == lane, positions[...].astype(F32), 0.0), axis=1, keepdims=True)
    angles = (pos_col * (1.0 / ROPE_FACTOR)) * freq[...]
    cos_part = jnp.cos(angles)
    half = lax.broadcasted_iota(jnp.int32, (rows, HD), 1) < HD // 2
    sin_part = jnp.where(half, -jnp.sin(angles), jnp.sin(angles))
    len_row = jnp.concatenate([lengths[...]] * heads + [jnp.zeros((1, HD // 2 - heads * rows), jnp.int32)] * (heads * rows < HD // 2), axis=1)
    len_row = jnp.concatenate([len_row, len_row], axis=1)
    own_rows = lax.broadcasted_iota(jnp.int32, (rows, LANES), 0)
    for tile in range(width // LANES):
        block = tokens[:, tile * LANES : (tile + 1) * LANES].astype(F32)
        for i in range(mine):
            tok_mine[i : i + 1, tile * LANES : (tile + 1) * LANES] = jnp.sum(
                jnp.where(own_rows == me_t * mine + i, block, 0.0), axis=0, keepdims=True
            )
    for copy in c_w:
        copy.wait()

    group = max(dp // 2, 1)
    own_part = None
    part_rows = rows // 2
    second_copies, other_copies = [[None] * dp for _ in range(2)], [None] * dp

    def send_part(n, k):
        second_copies[n][k] = send(
            part_out.at[n, k], part_in.at[n, k], s2.at[n, k], r2.at[n, k], {"dp": plane_source(plane[k])}
        )

    for g0 in reversed(range(0, dp, group)):
        for k in range(max(g0, 1), g0 + group):
            first_copies[k].wait_recv()
        lhs = spread[g0 : g0 + group].reshape(group * rows, share_pad)
        part = jnp.dot(lhs, weights[...], preferred_element_type=F32)
        if g0 == 0:
            own_part = part[:rows]
        sent = part.astype(BF16).reshape(group, rows, part.shape[1])
        other_out[g0 : g0 + group] = sent[:, :, q_cols:]
        for k in reversed(range(max(g0, 1), g0 + group)):
            for n in range(2):
                first = (k - g0) * rows + n * part_rows
                part_out[n, k] = part[first : first + part_rows, :q_cols].astype(BF16)
        for k in reversed(range(max(g0, 1), g0 + group)):
            send_part(0, k)
    for k in reversed(range(1, dp)):
        send_part(1, k)
    for k in reversed(range(1, dp)):
        other_copies[k] = send(
            other_out.at[k], other_in.at[k], s2.at[2, k], r2.at[2, k], {"dp": plane_source(plane[k])}
        )

    def rms_rope(vectors, gain, first):
        count = vectors.shape[0]
        square = jnp.sum(vectors * vectors, axis=1, keepdims=True) * (1.0 / HD)
        scaled = vectors * lax.rsqrt(square + EPS) * gain
        return (
            scaled * cos_part[first : first + count]
            + pltpu.roll(scaled, HD // 2, 1) * sin_part[first : first + count]
        )

    def queries_of(n):
        first = n * part_rows
        joined = own_part[first : first + part_rows, :q_cols]
        for k in range(1, dp):
            second_copies[n][k].wait_recv()
            joined = joined + part_in[n, k].astype(F32)
        zeros_part = jnp.zeros((part_rows, HD), F32)
        stacked = []
        for h in range(heads):
            query = rms_rope(joined[:, h * HD : (h + 1) * HD], q_gain[...], first) * QPRE ** (-0.5)
            both = jnp.concatenate([zeros_part, query] if n else [query, zeros_part], axis=0)
            nothing = jnp.zeros((rows, HD), F32)
            stacked.append(jnp.concatenate([both if g == h // per_kv else nothing for g in range(kv_heads)], axis=1))
        if heads * rows < HD // 2:
            stacked.append(jnp.zeros((HD // 2 - heads * rows, kv_cols), F32))
        return jnp.concatenate(stacked, axis=0).astype(BF16)

    half_rows = HD // 2
    query_of = lax.broadcasted_iota(jnp.int32, (half_rows, 1), 0) % rows
    zeros_half = jnp.zeros((half_rows, kv_cols), BF16)
    picks = [(query_of == b).astype(F32).astype(BF16) for b in range(rows)]
    contract_last = (((1,), (1,)), ((), ()))
    for copy in c_k:
        copy.wait()
    slots_half = ctx // 2
    block_rows = min(256, slots_half)
    blocks = slots_half // block_rows
    lane_row = lax.broadcasted_iota(jnp.int32, (1, HD), 1)
    base_slot = jnp.where(lane_row < half_rows, 0, slots_half)

    def scores_of(query_part, n, m):
        total = None
        for b in range(n * part_rows, (n + 1) * part_rows):
            only = query_part * picks[b]
            for high in range(2):
                first = high * slots_half + m * block_rows
                one = lax.dot_general(
                    kcache[b, first : first + block_rows, :],
                    jnp.concatenate([zeros_half, only] if high else [only, zeros_half], axis=0),
                    contract_last, preferred_element_type=F32,
                )
                total = one if total is None else total + one
        return total

    query_parts = [queries_of(0)]
    for copy in early_copies:
        copy.wait_recv()
    late_copies = []
    for way, (step, first, count) in enumerate(ways):
        piece = rows_of(jnp.where(first_core, ys[-step], xs[-step]), first, count)
        late_copies.append(send(piece, piece, sw.at[way, 1], rw.at[way, 1], {"dp": gather_peer(step)}))
        piece = rows_of(across, *ways[1 - way][1:])
        late_copies.append(send(piece, piece, sw.at[way, 2], rw.at[way, 2], {"dp": gather_peer(step)}))

    for m in range(blocks):
        scores[m * block_rows : (m + 1) * block_rows, :] = scores_of(query_parts[0], 0, m)
    query_parts.append(queries_of(1))
    query_rows = query_parts[0] + query_parts[1]
    largest = None
    for m in range(blocks):
        slot = lax.broadcasted_iota(jnp.int32, (block_rows, HD), 0) + (m * block_rows) + base_slot
        total = scores[m * block_rows : (m + 1) * block_rows, :] + scores_of(query_parts[1], 1, m)
        total = jnp.where(slot < len_row, total, -jnp.inf)
        scores[m * block_rows : (m + 1) * block_rows, :] = total
        top = jnp.max(total, axis=0, keepdims=True)
        largest = top if largest is None else jnp.maximum(largest, top)
    others = own_part[:, q_cols:]
    for k in range(1, dp):
        other_copies[k].wait_recv()
        others = others + other_in[k].astype(F32)
    new_keys = jnp.concatenate(
        [rms_rope(others[:, g * HD : (g + 1) * HD], k_gain[...], 0) for g in range(kv_heads)], axis=1
    ).astype(BF16)
    new_values = others[:, kv_cols:].astype(BF16)
    nk_out[...] = new_keys
    nv_out[...] = new_values

    own_scores = lax.dot_general(
        new_keys, jnp.concatenate([query_rows, query_rows], axis=0), contract_last, preferred_element_type=F32
    )
    own_lane = lax.broadcasted_iota(jnp.int32, (rows, HD), 1) % rows
    own_diag = lax.broadcasted_iota(jnp.int32, (rows, HD), 0) == own_lane
    own_row = jnp.sum(jnp.where(own_diag, own_scores, 0.0), axis=0, keepdims=True)
    largest = jnp.maximum(jnp.maximum(largest, pltpu.roll(largest, half_rows, 1)), own_row)
    own_weight = jnp.exp(own_row - largest)
    total_row = None
    for m in range(blocks):
        weight = jnp.exp(scores[m * block_rows : (m + 1) * block_rows, :] - largest)
        part_total = jnp.sum(weight, axis=0, keepdims=True)
        total_row = part_total if total_row is None else total_row + part_total
        probs[:, m * block_rows : (m + 1) * block_rows] = weight.T.astype(BF16)
    total_row = total_row + pltpu.roll(total_row, half_rows, 1) + own_weight
    eye = lax.broadcasted_iota(jnp.int32, (half_rows, HD), 0) == lax.broadcasted_iota(jnp.int32, (half_rows, HD), 1)
    total_col = jnp.sum(jnp.where(eye, total_row, 0.0), axis=1, keepdims=True)
    own_mix = jnp.where(own_diag, own_weight, 0.0)[:, :half_rows].astype(BF16)
    mixture = lax.dot_general(own_mix, new_values, (((0,), (0,)), ((), ())), preferred_element_type=F32)
    for copy in c_v:
        copy.wait()
    low_p = probs[:half_rows, :]
    high_p = probs[half_rows:, :]
    for b in range(rows):
        mixture = mixture + jnp.dot(low_p * picks[b], vcache[b, :slots_half, :], preferred_element_type=F32)
        mixture = mixture + jnp.dot(high_p * picks[b], vcache[b, slots_half:, :], preferred_element_type=F32)
    mixture = mixture / total_col
    attended = jnp.concatenate(
        [mixture[h * rows : (h + 1) * rows, (h // per_kv) * HD : (h // per_kv + 1) * HD] for h in range(heads)], axis=1
    ).astype(BF16)

    att_in[0] = attended
    third_copies = [None] * side
    for k in reversed(range(1, side)):
        third_copies[k] = send(
            att_in.at[0], att_in.at[k], s3.at[k], r3.at[k], {"dp": spread_peer(ring[k])}
        )
    for copy in late_copies:
        copy.wait_recv()
    for k in range(1, side):
        third_copies[k].wait_recv()
    products = lax.dot_general(
        att_in[...].reshape(side * rows, q_cols), oweight[...], contract_last, preferred_element_type=F32
    ).astype(BF16)

    for k in range(side):
        for t in range(tensor):
            first = k * rows + t * mine
            red_out[k, t] = products[first : first + mine, :]
    fourth_copies = []
    for k in reversed(range(side)):
        for turn, (step_z, step_c) in reversed(list(enumerate(line))):
            if k or turn:
                peer_t = line_peer((step_z, step_c))
                slot = red_in.at[my_c, place, step_z]
                fourth_copies.append(
                    send(
                        red_out.at[k, peer_t], slot, s4.at[k, turn], r4.at[k, turn],
                        {"dp": spread_peer(-ring[k] % side), "tensor": peer_t},
                    )
                )
    red_in[my_c, place, 0] = red_out[0, me_t]
    for copy in fourth_copies:
        copy.wait_recv()
    tiles = [jnp.zeros((mine, LANES), F32) for _ in range(width // LANES)]
    lane_pair = lax.broadcasted_iota(jnp.int32, (mine, LANES), 1)
    for d in range(dp):
        parts = []
        for c, p, a in ((0, d // side, d % side), (1, d % side, d // side)):
            for z in range(depth):
                parts.append(red_in[c, p, z, :, a * share_pad : (a + 1) * share_pad].astype(F32))
        while len(parts) > 1:
            parts = [parts[n] + parts[n + 1] for n in range(0, len(parts) - 1, 2)] + parts[len(parts) // 2 * 2 :]
        low, turn = share * d // LANES, share * d % LANES
        columns = [parts[0][:, n * LANES : (n + 1) * LANES] for n in range(share_pad // LANES)]
        if turn:
            columns = [pltpu.roll(column, turn, 1) for column in columns]
            none = jnp.zeros((mine, LANES), F32)
            columns = [
                jnp.where(lane_pair < turn, before, after)
                for before, after in zip([none] + columns, columns + [none])
            ]
        for n, column in enumerate(columns):
            if low + n < len(tiles) and n * LANES < turn + share:
                tiles[low + n] = tiles[low + n] + column
    square = tiles[0] * tiles[0]
    for tile in tiles[1:]:
        square = square + tile * tile
    scale = lax.rsqrt(jnp.sum(square, axis=1, keepdims=True) * (1.0 / width) + EPS)
    projected = jnp.concatenate(tiles, axis=1)
    row_out[...] = (tok_mine[...] + projected * scale * post_gain[...]).astype(BF16)

    keep = pltpu.make_async_copy(row_out, hid_hbm.at[me_t], last_sem)
    keep.start()
    fifth_copies = [
        send(row_out, hid_hbm.at[me_t], s5.at[k], r5.at[k], {"tensor": line_peer(line[k])})
        for k in reversed(range(1, tensor))
    ]
    for copy in sends:
        copy.wait_send()
    keep.wait()
    for copy in fifth_copies:
        copy.wait_recv()


def finish_kernel(hid_in, nk_in, nv_in, hid, nk, nv):
    hid[...] = hid_in[...].reshape(hid.shape)
    nk[...] = nk_in[...]
    nv[...] = nv_in[...]


def per_device(dp, tensor, side, *args):
    tokens, lengths, positions, in_gain, qw, kw, vw, q_gain, k_gain, kc, vc, ow, post_gain = args
    rows, width = tokens.shape
    share, q_cols = qw.shape
    kv_cols = kw.shape[1]
    ctx = kc.shape[1]
    share_pad = padded(share)
    cols = q_cols + 2 * kv_cols
    mine = rows // tensor
    depth = tensor // 2
    strip = side * share_pad
    dims = (dp, tensor, side, rows, width, share, q_cols, kv_cols, ctx, strip)
    exponent = np.arange(HD // 2, dtype=np.float64) * (2.0 / HD)
    frequency = (ROPE_BASE**-exponent).astype(np.float32)
    freq = jnp.asarray(np.concatenate([frequency, frequency])[None])
    any_spec = pl.BlockSpec(memory_space=pl.ANY)
    vmem_spec = pl.BlockSpec(memory_space=pltpu.VMEM)
    dma = pltpu.SemaphoreType.DMA
    hidden, new_keys, new_values = pl.pallas_call(
        functools.partial(kernel, dims),
        out_shape=(
            jax.ShapeDtypeStruct((tensor, mine, width), BF16),
            jax.ShapeDtypeStruct((rows, kv_cols), BF16),
            jax.ShapeDtypeStruct((rows, kv_cols), BF16),
        ),
        in_specs=[any_spec] * 14,
        out_specs=(any_spec, vmem_spec, vmem_spec),
        scratch_shapes=[
            pltpu.VMEM((rows, width), BF16),
            pltpu.VMEM((1, rows), jnp.int32),
            pltpu.VMEM((1, rows), jnp.int32),
            pltpu.VMEM((1, width), F32),
            pltpu.VMEM((share_pad, cols), BF16),
            pltpu.VMEM((1, HD), F32),
            pltpu.VMEM((1, HD), F32),
            pltpu.VMEM((rows, ctx, kv_cols), BF16),
            pltpu.VMEM((rows, ctx, kv_cols), BF16),
            pltpu.VMEM((strip, q_cols), BF16),
            pltpu.VMEM((1, width), F32),
            pltpu.VMEM((1, HD), F32),
            pltpu.VMEM((rows, width + 2 * LANES), F32),
            pltpu.VMEM((mine, width), F32),
            pltpu.VMEM((dp, rows, share_pad), BF16),
            pltpu.VMEM((dp, rows, share_pad), BF16),
            pltpu.VMEM((2, dp, rows // 2, q_cols), BF16),
            pltpu.VMEM((2, dp, rows // 2, q_cols), BF16),
            pltpu.VMEM((dp, rows, 2 * kv_cols), BF16),
            pltpu.VMEM((dp, rows, 2 * kv_cols), BF16),
            pltpu.VMEM((ctx // 2, HD), F32),
            pltpu.VMEM((HD, ctx // 2), BF16),
            pltpu.VMEM((side, rows, q_cols), BF16),
            pltpu.VMEM((side, tensor, mine, strip), BF16),
            pltpu.VMEM((2, side, depth, mine, strip), BF16),
            pltpu.VMEM((mine, width), BF16),
            dma((12,)),
            dma((2, rows)),
            dma((dp,)), dma((dp,)),
            dma((3, dp)), dma((3, dp)),
            dma((side,)), dma((side,)),
            dma((side, tensor)), dma((side, tensor)),
            dma((tensor,)), dma((tensor,)),
            dma((2, 3)), dma((2, 3)),
            dma(()),
        ],
        compiler_params=pltpu.CompilerParams(collective_id=0, has_side_effects=True, vmem_limit_bytes=50 * 1024 * 1024),
    )(
        *[
            pltpu.with_memory_space_constraint(operand, pltpu.HBM)
            for operand in (
                tokens, lengths.reshape(1, rows), positions.reshape(1, rows), in_gain, qw, kw, vw,
                q_gain.reshape(1, HD), k_gain.reshape(1, HD), kc, vc, ow.T, post_gain, freq,
            )
        ]
    )
    return pl.pallas_call(
        finish_kernel,
        out_shape=(
            jax.ShapeDtypeStruct((rows, width), BF16),
            jax.ShapeDtypeStruct((rows, kv_cols), BF16),
            jax.ShapeDtypeStruct((rows, kv_cols), BF16),
        ),
        compiler_params=pltpu.CompilerParams(vmem_limit_bytes=4 * 1024 * 1024),
    )(hidden, new_keys, new_values)


def solution(mesh):
    dp, tensor = mesh.shape["dp"], mesh.shape["tensor"]
    side = int(round(dp**0.5))
    return jax.shard_map(
        functools.partial(per_device, dp, tensor, side),
        mesh=mesh,
        in_specs=(
            P("dp", None), P("dp"), P("dp"), P(), P("dp", "tensor"), P("dp", "tensor"), P("dp", "tensor"), P(), P(),
            P("dp", None, "tensor"), P("dp", None, "tensor"), P("tensor", "dp"), P(),
        ),
        out_specs=(P("dp", None), P("dp", "tensor"), P("dp", "tensor")),
        check_vma=False,
    )
```

```python
import functools

import jax
import jax.numpy as jnp
import numpy as np
from jax import lax
from jax.experimental import pallas as pl
from jax.experimental.pallas import tpu as pltpu
from jax.sharding import PartitionSpec as P

HD = 128
QPRE = 168
LANES = 128
EPS = 1e-06
ROPE_BASE = 1000000.0
ROPE_FACTOR = 8.0
MESH = pl.DeviceIdType.MESH
F32 = jnp.float32
BF16 = jnp.bfloat16


def padded(width):
    return -(-width // LANES) * LANES


def ring_distance(step, size):
    return min(step % size, -step % size)


def plane_offsets(side):
    steps = [(a, b) for a in range(side) for b in range(side)]
    return sorted(steps, key=lambda s: (ring_distance(s[0], side) + ring_distance(s[1], side), s))


def line_offsets(depth):
    steps = [(a, c) for a in range(depth) for c in range(2)]
    return sorted(steps, key=lambda s: (ring_distance(s[0], depth), s[1]))


def kernel(
    dims,
    tokens_hbm, lengths_hbm, positions_hbm, in_gain_hbm, qw_hbm, kw_hbm, vw_hbm, q_gain_hbm, k_gain_hbm,
    kc_hbm, vc_hbm, ow_hbm, post_gain_hbm, freq_hbm,
    hid_hbm, nk_out, nv_out,
    tokens, lengths, positions, in_gain, weights, q_gain, k_gain, kcache, vcache, oweight, post_gain, freq,
    normed, tok_mine, slots, spread, part_out, part_in, other_out, other_in, scores, probs, att_in, red_out, red_in, row_out,
    load_sem, cache_sem, s1, r1, s2, r2, s3, r3, s4, r4, s5, r5, sw, rw, last_sem,
):
    dp, tensor, side, rows, width, share, q_cols, kv_cols, ctx, strip = dims
    depth = tensor // 2
    mine = rows // tensor
    heads = q_cols // HD
    kv_heads = kv_cols // HD
    per_kv = heads // kv_heads
    share_pad = padded(share)
    me = lax.axis_index("dp")
    me_t = lax.axis_index("tensor")
    my_x, my_y = lax.div(me, side), lax.rem(me, side)
    my_z, my_c = lax.div(me_t, 2), lax.rem(me_t, 2)
    xs = [my_x] + [lax.rem(my_x + a, side) for a in range(1, side)]
    ys = [my_y] + [lax.rem(my_y + a, side) for a in range(1, side)]
    zs = [my_z] + [lax.rem(my_z + a, depth) for a in range(1, depth)]
    cs = [my_c, 1 - my_c]

    def plane_peer(step):
        return xs[step[0]] * side + ys[step[1]]

    def plane_source(step):
        return xs[-step[0]] * side + ys[-step[1]]

    first_core = my_c == 0
    place = jnp.where(first_core, my_x, my_y)
    across = jnp.where(first_core, my_y, my_x)
    along_x = [xs[a] * side + my_y for a in range(side)]
    along_y = [my_x * side + ys[a] for a in range(side)]

    def gather_peer(a):
        return jnp.where(first_core, along_y[a], along_x[a])

    def spread_peer(a):
        return jnp.where(first_core, along_x[a], along_y[a])

    def line_peer(step):
        return zs[step[0]] * 2 + cs[step[1]]

    plane = plane_offsets(side)
    line = line_offsets(depth)
    ring = sorted(range(side), key=lambda a: (ring_distance(a, side), a))

    for a in range(side):
        oweight[a * share_pad + share : (a + 1) * share_pad, :] = jnp.zeros((share_pad - share, q_cols), BF16)

    barrier = pltpu.get_barrier_semaphore()
    greeted = [({"dp": plane_peer(step)}) for step in reversed(plane[1:])]
    for step in reversed(line[1:]):
        greeted.append({"tensor": line_peer(step)})
        for a in range(1, side):
            if step[1]:
                greeted.append({"dp": along_x[a], "tensor": line_peer(step)})
                greeted.append({"dp": along_y[a], "tensor": line_peer(step)})
            else:
                greeted.append({"dp": spread_peer(a), "tensor": line_peer(step)})
    for device in greeted:
        pl.semaphore_signal(barrier, inc=1, device_id=device, device_id_type=MESH)

    def load(src, dst, at):
        copy = pltpu.make_async_copy(src, dst, load_sem.at[at])
        copy.start()
        return copy

    c_tokens = load(tokens_hbm, tokens, 0)
    c_gain = load(in_gain_hbm, in_gain.at[0], 1)
    c_w = [
        load(qw_hbm, weights.at[pl.ds(0, share), pl.ds(0, q_cols)], 2),
        load(kw_hbm, weights.at[pl.ds(0, share), pl.ds(q_cols, kv_cols)], 3),
        load(vw_hbm, weights.at[pl.ds(0, share), pl.ds(q_cols + kv_cols, kv_cols)], 4),
    ]
    c_small = [
        load(lengths_hbm, lengths, 5), load(positions_hbm, positions, 6), load(q_gain_hbm, q_gain, 7),
        load(k_gain_hbm, k_gain, 8), load(post_gain_hbm, post_gain.at[0], 9), load(freq_hbm, freq, 10),
    ]
    def rows_of(at, first, count):
        return oweight.at[pl.ds(pl.multiple_of(at * share_pad + first, 16), count), :]

    own_block = rows_of(across, 0, share)
    c_ow = load(ow_hbm, own_block, 11)

    c_tokens.wait()
    c_gain.wait()
    x = tokens[...].astype(F32)
    mean_square = jnp.sum(x * x, axis=1, keepdims=True) * (1.0 / width)
    normed[:, :width] = x * lax.rsqrt(mean_square + EPS) * in_gain[...]
    normed[:, width:] = jnp.zeros((rows, normed.shape[1] - width), F32)
    for d in range(dp):
        first = share * d
        low = first // LANES * LANES
        window = normed[:, low : low + share_pad + LANES]
        if first != low:
            window = pltpu.roll(window, window.shape[1] - (first - low), 1)
        slots[d] = window[:, :share_pad].astype(BF16)

    pl.semaphore_wait(barrier, len(greeted))

    sends = []

    def send(src, dst, send_sem, recv_sem, device):
        copy = pltpu.make_async_remote_copy(
            src_ref=src, dst_ref=dst, send_sem=send_sem, recv_sem=recv_sem, device_id=device, device_id_type=MESH
        )
        copy.start()
        sends.append(copy)
        return copy

    first_copies = [None] * dp
    for k in reversed(range(1, dp)):
        peer = plane_peer(plane[k])
        first_copies[k] = send(slots.at[peer], spread.at[k], s1.at[k], r1.at[k], {"dp": peer})
    spread[0] = slots[me]
    far = -(-share // 32) * 16
    c_ow.wait()
    ways = ((1, 0, far), (side - 1, far, share - far))
    early_copies = []
    for way, (step, first, count) in enumerate(ways):
        piece = rows_of(across, first, count)
        early_copies.append(send(piece, piece, sw.at[way, 0], rw.at[way, 0], {"dp": gather_peer(step)}))

    c_k, c_v = [], []
    for b in range(rows):
        copy = pltpu.make_async_copy(kc_hbm.at[b], kcache.at[b], cache_sem.at[0, b])
        copy.start()
        c_k.append(copy)
    for b in range(rows):
        copy = pltpu.make_async_copy(vc_hbm.at[b], vcache.at[b], cache_sem.at[1, b])
        copy.start()
        c_v.append(copy)

    weights[share:, :] = jnp.zeros((share_pad - share, weights.shape[1]), BF16)
    for copy in c_small:
        copy.wait()
    sub = lax.broadcasted_iota(jnp.int32, (rows, rows), 0)
    lane = lax.broadcasted_iota(jnp.int32, (rows, rows), 1)
    pos_col = jnp.sum(jnp.where(sub == lane, positions[...].astype(F32), 0.0), axis=1, keepdims=True)
    angles = (pos_col * (1.0 / ROPE_FACTOR)) * freq[...]
    cos_part = jnp.cos(angles)
    half = lax.broadcasted_iota(jnp.int32, (rows, HD), 1) < HD // 2
    sin_part = jnp.where(half, -jnp.sin(angles), jnp.sin(angles))
    len_row = jnp.concatenate([lengths[...]] * heads + [jnp.zeros((1, HD // 2 - heads * rows), jnp.int32)] * (heads * rows < HD // 2), axis=1)
    len_row = jnp.concatenate([len_row, len_row], axis=1)
    own_rows = lax.broadcasted_iota(jnp.int32, (rows, LANES), 0)
    for tile in range(width // LANES):
        block = tokens[:, tile * LANES : (tile + 1) * LANES].astype(F32)
        for i in range(mine):
            tok_mine[i : i + 1, tile * LANES : (tile + 1) * LANES] = jnp.sum(
                jnp.where(own_rows == me_t * mine + i, block, 0.0), axis=0, keepdims=True
            )
    for copy in c_w:
        copy.wait()

    group = max(dp // 2, 1)
    own_part = None
    part_rows = rows // 2
    second_copies, other_copies = [[None] * dp for _ in range(2)], [None] * dp

    def send_part(n, k):
        second_copies[n][k] = send(
            part_out.at[n, k], part_in.at[n, k], s2.at[n, k], r2.at[n, k], {"dp": plane_source(plane[k])}
        )

    for g0 in reversed(range(0, dp, group)):
        for k in range(max(g0, 1), g0 + group):
            first_copies[k].wait_recv()
        lhs = spread[g0 : g0 + group].reshape(group * rows, share_pad)
        part = jnp.dot(lhs, weights[:, :q_cols], preferred_element_type=F32)
        if g0 == 0:
            own_part = part[:rows]
        for k in reversed(range(max(g0, 1), g0 + group)):
            for n in range(2):
                first = (k - g0) * rows + n * part_rows
                part_out[n, k] = part[first : first + part_rows, :q_cols].astype(BF16)
        for k in reversed(range(max(g0, 1), g0 + group)):
            send_part(0, k)
    for k in reversed(range(1, dp)):
        send_part(1, k)
    other = jnp.dot(spread[...].reshape(dp * rows, share_pad), weights[:, q_cols:], preferred_element_type=F32)
    own_other = other[:rows]
    other_out[...] = other.astype(BF16).reshape(other_out.shape)
    for k in reversed(range(1, dp)):
        other_copies[k] = send(
            other_out.at[k], other_in.at[k], s2.at[2, k], r2.at[2, k], {"dp": plane_source(plane[k])}
        )

    def rms_rope(vectors, gain, first):
        count = vectors.shape[0]
        square = jnp.sum(vectors * vectors, axis=1, keepdims=True) * (1.0 / HD)
        scaled = vectors * lax.rsqrt(square + EPS) * gain
        return (
            scaled * cos_part[first : first + count]
            + pltpu.roll(scaled, HD // 2, 1) * sin_part[first : first + count]
        )

    def queries_of(n):
        first = n * part_rows
        joined = own_part[first : first + part_rows, :q_cols]
        for k in range(1, dp):
            second_copies[n][k].wait_recv()
            joined = joined + part_in[n, k].astype(F32)
        zeros_part = jnp.zeros((part_rows, HD), F32)
        stacked = []
        for h in range(heads):
            query = rms_rope(joined[:, h * HD : (h + 1) * HD], q_gain[...], first) * QPRE ** (-0.5)
            both = jnp.concatenate([zeros_part, query] if n else [query, zeros_part], axis=0)
            nothing = jnp.zeros((rows, HD), F32)
            stacked.append(jnp.concatenate([both if g == h // per_kv else nothing for g in range(kv_heads)], axis=1))
        if heads * rows < HD // 2:
            stacked.append(jnp.zeros((HD // 2 - heads * rows, kv_cols), F32))
        return jnp.concatenate(stacked, axis=0).astype(BF16)

    half_rows = HD // 2
    query_of = lax.broadcasted_iota(jnp.int32, (half_rows, 1), 0) % rows
    zeros_half = jnp.zeros((half_rows, kv_cols), BF16)
    picks = [(query_of == b).astype(F32).astype(BF16) for b in range(rows)]
    contract_last = (((1,), (1,)), ((), ()))
    for copy in c_k:
        copy.wait()
    slots_half = ctx // 2
    block_rows = min(256, slots_half)
    blocks = slots_half // block_rows
    lane_row = lax.broadcasted_iota(jnp.int32, (1, HD), 1)
    base_slot = jnp.where(lane_row < half_rows, 0, slots_half)

    def scores_of(query_part, n, m):
        total = None
        for b in range(n * part_rows, (n + 1) * part_rows):
            only = query_part * picks[b]
            for high in range(2):
                first = high * slots_half + m * block_rows
                one = lax.dot_general(
                    kcache[b, first : first + block_rows, :],
                    jnp.concatenate([zeros_half, only] if high else [only, zeros_half], axis=0),
                    contract_last, preferred_element_type=F32,
                )
                total = one if total is None else total + one
        return total

    query_parts = [queries_of(0)]
    for copy in early_copies:
        copy.wait_recv()
    late_copies = []
    for way, (step, first, count) in enumerate(ways):
        piece = rows_of(jnp.where(first_core, ys[-step], xs[-step]), first, count)
        late_copies.append(send(piece, piece, sw.at[way, 1], rw.at[way, 1], {"dp": gather_peer(step)}))
        piece = rows_of(across, *ways[1 - way][1:])
        late_copies.append(send(piece, piece, sw.at[way, 2], rw.at[way, 2], {"dp": gather_peer(step)}))

    for m in range(blocks):
        scores[m * block_rows : (m + 1) * block_rows, :] = scores_of(query_parts[0], 0, m)
    query_parts.append(queries_of(1))
    query_rows = query_parts[0] + query_parts[1]
    largest = None
    for m in range(blocks):
        slot = lax.broadcasted_iota(jnp.int32, (block_rows, HD), 0) + (m * block_rows) + base_slot
        total = scores[m * block_rows : (m + 1) * block_rows, :] + scores_of(query_parts[1], 1, m)
        total = jnp.where(slot < len_row, total, -jnp.inf)
        scores[m * block_rows : (m + 1) * block_rows, :] = total
        top = jnp.max(total, axis=0, keepdims=True)
        largest = top if largest is None else jnp.maximum(largest, top)
    others = own_other
    for k in range(1, dp):
        other_copies[k].wait_recv()
        others = others + other_in[k].astype(F32)
    new_keys = jnp.concatenate(
        [rms_rope(others[:, g * HD : (g + 1) * HD], k_gain[...], 0) for g in range(kv_heads)], axis=1
    ).astype(BF16)
    new_values = others[:, kv_cols:].astype(BF16)
    nk_out[...] = new_keys
    nv_out[...] = new_values

    own_scores = lax.dot_general(
        new_keys, jnp.concatenate([query_rows, query_rows], axis=0), contract_last, preferred_element_type=F32
    )
    own_lane = lax.broadcasted_iota(jnp.int32, (rows, HD), 1) % rows
    own_diag = lax.broadcasted_iota(jnp.int32, (rows, HD), 0) == own_lane
    own_row = jnp.sum(jnp.where(own_diag, own_scores, 0.0), axis=0, keepdims=True)
    largest = jnp.maximum(jnp.maximum(largest, pltpu.roll(largest, half_rows, 1)), own_row)
    own_weight = jnp.exp(own_row - largest)
    total_row = None
    for m in range(blocks):
        weight = jnp.exp(scores[m * block_rows : (m + 1) * block_rows, :] - largest)
        part_total = jnp.sum(weight, axis=0, keepdims=True)
        total_row = part_total if total_row is None else total_row + part_total
        probs[:, m * block_rows : (m + 1) * block_rows] = weight.T.astype(BF16)
    total_row = total_row + pltpu.roll(total_row, half_rows, 1) + own_weight
    eye = lax.broadcasted_iota(jnp.int32, (half_rows, HD), 0) == lax.broadcasted_iota(jnp.int32, (half_rows, HD), 1)
    total_col = jnp.sum(jnp.where(eye, total_row, 0.0), axis=1, keepdims=True)
    own_mix = jnp.where(own_diag, own_weight, 0.0)[:, :half_rows].astype(BF16)
    mixture = lax.dot_general(own_mix, new_values, (((0,), (0,)), ((), ())), preferred_element_type=F32)
    for copy in c_v:
        copy.wait()
    low_p = probs[:half_rows, :]
    high_p = probs[half_rows:, :]
    for b in range(rows):
        mixture = mixture + jnp.dot(low_p * picks[b], vcache[b, :slots_half, :], preferred_element_type=F32)
        mixture = mixture + jnp.dot(high_p * picks[b], vcache[b, slots_half:, :], preferred_element_type=F32)
    mixture = mixture / total_col
    attended = jnp.concatenate(
        [mixture[h * rows : (h + 1) * rows, (h // per_kv) * HD : (h // per_kv + 1) * HD] for h in range(heads)], axis=1
    ).astype(BF16)

    att_in[0] = attended
    third_copies = [None] * side
    for k in reversed(range(1, side)):
        third_copies[k] = send(
            att_in.at[0], att_in.at[k], s3.at[k], r3.at[k], {"dp": spread_peer(ring[k])}
        )
    for copy in late_copies:
        copy.wait_recv()
    for k in range(1, side):
        third_copies[k].wait_recv()
    products = lax.dot_general(
        att_in[...].reshape(side * rows, q_cols), oweight[...], contract_last, preferred_element_type=F32
    ).astype(BF16)

    for k in range(side):
        for t in range(tensor):
            first = k * rows + t * mine
            red_out[k, t] = products[first : first + mine, :]
    fourth_copies = []
    for k in reversed(range(side)):
        for turn, (step_z, step_c) in reversed(list(enumerate(line))):
            if k or turn:
                peer_t = line_peer((step_z, step_c))
                slot = red_in.at[my_c, place, step_z]
                fourth_copies.append(
                    send(
                        red_out.at[k, peer_t], slot, s4.at[k, turn], r4.at[k, turn],
                        {"dp": spread_peer(-ring[k] % side), "tensor": peer_t},
                    )
                )
    red_in[my_c, place, 0] = red_out[0, me_t]
    for copy in fourth_copies:
        copy.wait_recv()
    tiles = [jnp.zeros((mine, LANES), F32) for _ in range(width // LANES)]
    lane_pair = lax.broadcasted_iota(jnp.int32, (mine, LANES), 1)
    for d in range(dp):
        parts = []
        for c, p, a in ((0, d // side, d % side), (1, d % side, d // side)):
            for z in range(depth):
                parts.append(red_in[c, p, z, :, a * share_pad : (a + 1) * share_pad].astype(F32))
        while len(parts) > 1:
            parts = [parts[n] + parts[n + 1] for n in range(0, len(parts) - 1, 2)] + parts[len(parts) // 2 * 2 :]
        low, turn = share * d // LANES, share * d % LANES
        columns = [parts[0][:, n * LANES : (n + 1) * LANES] for n in range(share_pad // LANES)]
        if turn:
            columns = [pltpu.roll(column, turn, 1) for column in columns]
            none = jnp.zeros((mine, LANES), F32)
            columns = [
                jnp.where(lane_pair < turn, before, after)
                for before, after in zip([none] + columns, columns + [none])
            ]
        for n, column in enumerate(columns):
            if low + n < len(tiles) and n * LANES < turn + share:
                tiles[low + n] = tiles[low + n] + column
    square = tiles[0] * tiles[0]
    for tile in tiles[1:]:
        square = square + tile * tile
    scale = lax.rsqrt(jnp.sum(square, axis=1, keepdims=True) * (1.0 / width) + EPS)
    projected = jnp.concatenate(tiles, axis=1)
    row_out[...] = (tok_mine[...] + projected * scale * post_gain[...]).astype(BF16)

    keep = pltpu.make_async_copy(row_out, hid_hbm.at[me_t], last_sem)
    keep.start()
    fifth_copies = [
        send(row_out, hid_hbm.at[me_t], s5.at[k], r5.at[k], {"tensor": line_peer(line[k])})
        for k in reversed(range(1, tensor))
    ]
    for copy in sends:
        copy.wait_send()
    keep.wait()
    for copy in fifth_copies:
        copy.wait_recv()


def finish_kernel(hid_in, nk_in, nv_in, hid, nk, nv):
    hid[...] = hid_in[...].reshape(hid.shape)
    nk[...] = nk_in[...]
    nv[...] = nv_in[...]


def per_device(dp, tensor, side, *args):
    tokens, lengths, positions, in_gain, qw, kw, vw, q_gain, k_gain, kc, vc, ow, post_gain = args
    rows, width = tokens.shape
    share, q_cols = qw.shape
    kv_cols = kw.shape[1]
    ctx = kc.shape[1]
    share_pad = padded(share)
    cols = q_cols + 2 * kv_cols
    mine = rows // tensor
    depth = tensor // 2
    strip = side * share_pad
    dims = (dp, tensor, side, rows, width, share, q_cols, kv_cols, ctx, strip)
    exponent = np.arange(HD // 2, dtype=np.float64) * (2.0 / HD)
    frequency = (ROPE_BASE**-exponent).astype(np.float32)
    freq = jnp.asarray(np.concatenate([frequency, frequency])[None])
    any_spec = pl.BlockSpec(memory_space=pl.ANY)
    vmem_spec = pl.BlockSpec(memory_space=pltpu.VMEM)
    dma = pltpu.SemaphoreType.DMA
    hidden, new_keys, new_values = pl.pallas_call(
        functools.partial(kernel, dims),
        out_shape=(
            jax.ShapeDtypeStruct((tensor, mine, width), BF16),
            jax.ShapeDtypeStruct((rows, kv_cols), BF16),
            jax.ShapeDtypeStruct((rows, kv_cols), BF16),
        ),
        in_specs=[any_spec] * 14,
        out_specs=(any_spec, vmem_spec, vmem_spec),
        scratch_shapes=[
            pltpu.VMEM((rows, width), BF16),
            pltpu.VMEM((1, rows), jnp.int32),
            pltpu.VMEM((1, rows), jnp.int32),
            pltpu.VMEM((1, width), F32),
            pltpu.VMEM((share_pad, cols), BF16),
            pltpu.VMEM((1, HD), F32),
            pltpu.VMEM((1, HD), F32),
            pltpu.VMEM((rows, ctx, kv_cols), BF16),
            pltpu.VMEM((rows, ctx, kv_cols), BF16),
            pltpu.VMEM((strip, q_cols), BF16),
            pltpu.VMEM((1, width), F32),
            pltpu.VMEM((1, HD), F32),
            pltpu.VMEM((rows, width + 2 * LANES), F32),
            pltpu.VMEM((mine, width), F32),
            pltpu.VMEM((dp, rows, share_pad), BF16),
            pltpu.VMEM((dp, rows, share_pad), BF16),
            pltpu.VMEM((2, dp, rows // 2, q_cols), BF16),
            pltpu.VMEM((2, dp, rows // 2, q_cols), BF16),
            pltpu.VMEM((dp, rows, 2 * kv_cols), BF16),
            pltpu.VMEM((dp, rows, 2 * kv_cols), BF16),
            pltpu.VMEM((ctx // 2, HD), F32),
            pltpu.VMEM((HD, ctx // 2), BF16),
            pltpu.VMEM((side, rows, q_cols), BF16),
            pltpu.VMEM((side, tensor, mine, strip), BF16),
            pltpu.VMEM((2, side, depth, mine, strip), BF16),
            pltpu.VMEM((mine, width), BF16),
            dma((12,)),
            dma((2, rows)),
            dma((dp,)), dma((dp,)),
            dma((3, dp)), dma((3, dp)),
            dma((side,)), dma((side,)),
            dma((side, tensor)), dma((side, tensor)),
            dma((tensor,)), dma((tensor,)),
            dma((2, 3)), dma((2, 3)),
            dma(()),
        ],
        compiler_params=pltpu.CompilerParams(collective_id=0, has_side_effects=True, vmem_limit_bytes=50 * 1024 * 1024),
    )(
        *[
            pltpu.with_memory_space_constraint(operand, pltpu.HBM)
            for operand in (
                tokens, lengths.reshape(1, rows), positions.reshape(1, rows), in_gain, qw, kw, vw,
                q_gain.reshape(1, HD), k_gain.reshape(1, HD), kc, vc, ow.T, post_gain, freq,
            )
        ]
    )
    return pl.pallas_call(
        finish_kernel,
        out_shape=(
            jax.ShapeDtypeStruct((rows, width), BF16),
            jax.ShapeDtypeStruct((rows, kv_cols), BF16),
            jax.ShapeDtypeStruct((rows, kv_cols), BF16),
        ),
        compiler_params=pltpu.CompilerParams(vmem_limit_bytes=4 * 1024 * 1024),
    )(hidden, new_keys, new_values)


def solution(mesh):
    dp, tensor = mesh.shape["dp"], mesh.shape["tensor"]
    side = int(round(dp**0.5))
    return jax.shard_map(
        functools.partial(per_device, dp, tensor, side),
        mesh=mesh,
        in_specs=(
            P("dp", None), P("dp"), P("dp"), P(), P("dp", "tensor"), P("dp", "tensor"), P("dp", "tensor"), P(), P(),
            P("dp", None, "tensor"), P("dp", None, "tensor"), P("tensor", "dp"), P(),
        ),
        out_specs=(P("dp", None), P("dp", "tensor"), P("dp", "tensor")),
        check_vma=False,
    )
```

```python
import functools

import jax
import jax.numpy as jnp
import numpy as np
from jax import lax
from jax.experimental import pallas as pl
from jax.experimental.pallas import tpu as pltpu
from jax.sharding import PartitionSpec as P

HD = 128
QPRE = 168
LANES = 128
EPS = 1e-06
ROPE_BASE = 1000000.0
ROPE_FACTOR = 8.0
MESH = pl.DeviceIdType.MESH
F32 = jnp.float32
BF16 = jnp.bfloat16


def padded(width):
    return -(-width // LANES) * LANES


def ring_distance(step, size):
    return min(step % size, -step % size)


def plane_offsets(side):
    steps = [(a, b) for a in range(side) for b in range(side)]
    return sorted(steps, key=lambda s: (ring_distance(s[0], side) + ring_distance(s[1], side), s))


def line_offsets(depth):
    steps = [(a, c) for a in range(depth) for c in range(2)]
    return sorted(steps, key=lambda s: (ring_distance(s[0], depth), s[1]))


def kernel(
    dims,
    tokens_hbm, lengths_hbm, positions_hbm, in_gain_hbm, qw_hbm, kw_hbm, vw_hbm, q_gain_hbm, k_gain_hbm,
    kc_hbm, vc_hbm, ow_hbm, post_gain_hbm, freq_hbm,
    hid_hbm, nk_out, nv_out,
    tokens, lengths, positions, in_gain, weights, q_gain, k_gain, kcache, vcache, oweight, post_gain, freq,
    normed, tok_mine, slots, spread, part_out, part_in, other_out, other_in, scores, probs, att_in, red_out, red_in, row_out,
    load_sem, cache_sem, s1, r1, s2, r2, s3, r3, s4, r4, s5, r5, sw, rw, last_sem,
):
    dp, tensor, side, rows, width, share, q_cols, kv_cols, ctx, strip = dims
    depth = tensor // 2
    mine = rows // tensor
    heads = q_cols // HD
    kv_heads = kv_cols // HD
    per_kv = heads // kv_heads
    share_pad = padded(share)
    me = lax.axis_index("dp")
    me_t = lax.axis_index("tensor")
    my_x, my_y = lax.div(me, side), lax.rem(me, side)
    my_z, my_c = lax.div(me_t, 2), lax.rem(me_t, 2)
    xs = [my_x] + [lax.rem(my_x + a, side) for a in range(1, side)]
    ys = [my_y] + [lax.rem(my_y + a, side) for a in range(1, side)]
    zs = [my_z] + [lax.rem(my_z + a, depth) for a in range(1, depth)]
    cs = [my_c, 1 - my_c]

    def plane_peer(step):
        return xs[step[0]] * side + ys[step[1]]

    def plane_source(step):
        return xs[-step[0]] * side + ys[-step[1]]

    first_core = my_c == 0
    place = jnp.where(first_core, my_x, my_y)
    across = jnp.where(first_core, my_y, my_x)
    along_x = [xs[a] * side + my_y for a in range(side)]
    along_y = [my_x * side + ys[a] for a in range(side)]

    def gather_peer(a):
        return jnp.where(first_core, along_y[a], along_x[a])

    def spread_peer(a):
        return jnp.where(first_core, along_x[a], along_y[a])

    def line_peer(step):
        return zs[step[0]] * 2 + cs[step[1]]

    plane = plane_offsets(side)
    line = line_offsets(depth)
    ring = sorted(range(side), key=lambda a: (ring_distance(a, side), a))


    barrier = pltpu.get_barrier_semaphore()
    greeted = [({"dp": plane_peer(step)}) for step in reversed(plane[1:])]
    for step in reversed(line[1:]):
        greeted.append({"tensor": line_peer(step)})
        for a in range(1, side):
            if step[1]:
                greeted.append({"dp": along_x[a], "tensor": line_peer(step)})
                greeted.append({"dp": along_y[a], "tensor": line_peer(step)})
            else:
                greeted.append({"dp": spread_peer(a), "tensor": line_peer(step)})
    for device in greeted:
        pl.semaphore_signal(barrier, inc=1, device_id=device, device_id_type=MESH)

    def load(src, dst, at):
        copy = pltpu.make_async_copy(src, dst, load_sem.at[at])
        copy.start()
        return copy

    c_tokens = load(tokens_hbm, tokens, 0)
    c_gain = load(in_gain_hbm, in_gain.at[0], 1)
    c_w = [
        load(qw_hbm, weights.at[pl.ds(0, share), pl.ds(0, q_cols)], 2),
        load(kw_hbm, weights.at[pl.ds(0, share), pl.ds(q_cols, kv_cols)], 3),
        load(vw_hbm, weights.at[pl.ds(0, share), pl.ds(q_cols + kv_cols, kv_cols)], 4),
    ]
    c_small = [
        load(lengths_hbm, lengths, 5), load(positions_hbm, positions, 6), load(q_gain_hbm, q_gain, 7),
        load(k_gain_hbm, k_gain, 8), load(post_gain_hbm, post_gain.at[0], 9), load(freq_hbm, freq, 10),
    ]
    def rows_of(at, first, count):
        return oweight.at[pl.ds(pl.multiple_of(at * share_pad + first, 16), count), :]

    own_block = rows_of(across, 0, share)
    c_ow = load(ow_hbm, own_block, 11)

    c_tokens.wait()
    c_gain.wait()
    x = tokens[...].astype(F32)
    mean_square = jnp.sum(x * x, axis=1, keepdims=True) * (1.0 / width)
    normed[:, :width] = x * lax.rsqrt(mean_square + EPS) * in_gain[...]
    normed[:, width:] = jnp.zeros((rows, normed.shape[1] - width), F32)
    for d in range(dp):
        first = share * d
        low = first // LANES * LANES
        window = normed[:, low : low + share_pad + LANES]
        if first != low:
            window = pltpu.roll(window, window.shape[1] - (first - low), 1)
        slots[d] = window[:, :share_pad].astype(BF16)

    pl.semaphore_wait(barrier, len(greeted))

    sends = []

    def send(src, dst, send_sem, recv_sem, device):
        copy = pltpu.make_async_remote_copy(
            src_ref=src, dst_ref=dst, send_sem=send_sem, recv_sem=recv_sem, device_id=device, device_id_type=MESH
        )
        copy.start()
        sends.append(copy)
        return copy

    first_copies = [None] * dp
    for k in reversed(range(1, dp)):
        peer = plane_peer(plane[k])
        first_copies[k] = send(slots.at[peer], spread.at[k], s1.at[k], r1.at[k], {"dp": peer})
    spread[0] = slots[me]
    far = -(-share // 32) * 16
    c_ow.wait()
    ways = ((1, 0, far), (side - 1, far, share - far))
    early_copies = []
    for way, (step, first, count) in enumerate(ways):
        piece = rows_of(across, first, count)
        early_copies.append(send(piece, piece, sw.at[way, 0], rw.at[way, 0], {"dp": gather_peer(step)}))

    c_k, c_v = [], []
    for b in range(rows):
        copy = pltpu.make_async_copy(kc_hbm.at[b], kcache.at[b], cache_sem.at[0, b])
        copy.start()
        c_k.append(copy)
    for b in range(rows):
        copy = pltpu.make_async_copy(vc_hbm.at[b], vcache.at[b], cache_sem.at[1, b])
        copy.start()
        c_v.append(copy)

    for a in range(side):
        oweight[a * share_pad + share : (a + 1) * share_pad, :] = jnp.zeros((share_pad - share, q_cols), BF16)
    weights[share:, :] = jnp.zeros((share_pad - share, weights.shape[1]), BF16)
    for copy in c_small:
        copy.wait()
    sub = lax.broadcasted_iota(jnp.int32, (rows, rows), 0)
    lane = lax.broadcasted_iota(jnp.int32, (rows, rows), 1)
    pos_col = jnp.sum(jnp.where(sub == lane, positions[...].astype(F32), 0.0), axis=1, keepdims=True)
    angles = (pos_col * (1.0 / ROPE_FACTOR)) * freq[...]
    cos_part = jnp.cos(angles)
    half = lax.broadcasted_iota(jnp.int32, (rows, HD), 1) < HD // 2
    sin_part = jnp.where(half, -jnp.sin(angles), jnp.sin(angles))
    len_row = jnp.concatenate([lengths[...]] * heads + [jnp.zeros((1, HD // 2 - heads * rows), jnp.int32)] * (heads * rows < HD // 2), axis=1)
    len_row = jnp.concatenate([len_row, len_row], axis=1)
    own_rows = lax.broadcasted_iota(jnp.int32, (rows, LANES), 0)
    for tile in range(width // LANES):
        block = tokens[:, tile * LANES : (tile + 1) * LANES].astype(F32)
        for i in range(mine):
            tok_mine[i : i + 1, tile * LANES : (tile + 1) * LANES] = jnp.sum(
                jnp.where(own_rows == me_t * mine + i, block, 0.0), axis=0, keepdims=True
            )
    for copy in c_w:
        copy.wait()

    group = max(dp // 2, 1)
    own_part = None
    part_rows = rows // 2
    second_copies, other_copies = [[None] * dp for _ in range(2)], [None] * dp

    def send_part(n, k):
        second_copies[n][k] = send(
            part_out.at[n, k], part_in.at[n, k], s2.at[n, k], r2.at[n, k], {"dp": plane_source(plane[k])}
        )

    for g0 in reversed(range(0, dp, group)):
        for k in range(max(g0, 1), g0 + group):
            first_copies[k].wait_recv()
        lhs = spread[g0 : g0 + group].reshape(group * rows, share_pad)
        part = jnp.dot(lhs, weights[:, :q_cols], preferred_element_type=F32)
        if g0 == 0:
            own_part = part[:rows]
        for k in reversed(range(max(g0, 1), g0 + group)):
            for n in range(2):
                first = (k - g0) * rows + n * part_rows
                part_out[n, k] = part[first : first + part_rows, :q_cols].astype(BF16)
        for k in reversed(range(max(g0, 1), g0 + group)):
            send_part(0, k)
    for k in reversed(range(1, dp)):
        send_part(1, k)
    other = jnp.dot(spread[...].reshape(dp * rows, share_pad), weights[:, q_cols:], preferred_element_type=F32)
    own_other = other[:rows]
    other_out[...] = other.astype(BF16).reshape(other_out.shape)
    for k in reversed(range(1, dp)):
        other_copies[k] = send(
            other_out.at[k], other_in.at[k], s2.at[2, k], r2.at[2, k], {"dp": plane_source(plane[k])}
        )

    def rms_rope(vectors, gain, first):
        count = vectors.shape[0]
        square = jnp.sum(vectors * vectors, axis=1, keepdims=True) * (1.0 / HD)
        scaled = vectors * lax.rsqrt(square + EPS) * gain
        return (
            scaled * cos_part[first : first + count]
            + pltpu.roll(scaled, HD // 2, 1) * sin_part[first : first + count]
        )

    def queries_of(n):
        first = n * part_rows
        joined = own_part[first : first + part_rows, :q_cols]
        for k in range(1, dp):
            second_copies[n][k].wait_recv()
            joined = joined + part_in[n, k].astype(F32)
        zeros_part = jnp.zeros((part_rows, HD), F32)
        stacked = []
        for h in range(heads):
            query = rms_rope(joined[:, h * HD : (h + 1) * HD], q_gain[...], first) * QPRE ** (-0.5)
            both = jnp.concatenate([zeros_part, query] if n else [query, zeros_part], axis=0)
            nothing = jnp.zeros((rows, HD), F32)
            stacked.append(jnp.concatenate([both if g == h // per_kv else nothing for g in range(kv_heads)], axis=1))
        if heads * rows < HD // 2:
            stacked.append(jnp.zeros((HD // 2 - heads * rows, kv_cols), F32))
        return jnp.concatenate(stacked, axis=0).astype(BF16)

    half_rows = HD // 2
    query_of = lax.broadcasted_iota(jnp.int32, (half_rows, 1), 0) % rows
    zeros_half = jnp.zeros((half_rows, kv_cols), BF16)
    picks = [(query_of == b).astype(F32).astype(BF16) for b in range(rows)]
    contract_last = (((1,), (1,)), ((), ()))
    for copy in c_k:
        copy.wait()
    slots_half = ctx // 2
    block_rows = min(256, slots_half)
    blocks = slots_half // block_rows
    lane_row = lax.broadcasted_iota(jnp.int32, (1, HD), 1)
    base_slot = jnp.where(lane_row < half_rows, 0, slots_half)

    def scores_of(query_part, n, m):
        total = None
        for b in range(n * part_rows, (n + 1) * part_rows):
            only = query_part * picks[b]
            for high in range(2):
                first = high * slots_half + m * block_rows
                one = lax.dot_general(
                    kcache[b, first : first + block_rows, :],
                    jnp.concatenate([zeros_half, only] if high else [only, zeros_half], axis=0),
                    contract_last, preferred_element_type=F32,
                )
                total = one if total is None else total + one
        return total

    query_parts = [queries_of(0)]
    for copy in early_copies:
        copy.wait_recv()
    late_copies = []
    for way, (step, first, count) in enumerate(ways):
        piece = rows_of(jnp.where(first_core, ys[-step], xs[-step]), first, count)
        late_copies.append(send(piece, piece, sw.at[way, 1], rw.at[way, 1], {"dp": gather_peer(step)}))
        piece = rows_of(across, *ways[1 - way][1:])
        late_copies.append(send(piece, piece, sw.at[way, 2], rw.at[way, 2], {"dp": gather_peer(step)}))

    for m in range(blocks):
        scores[m * block_rows : (m + 1) * block_rows, :] = scores_of(query_parts[0], 0, m)
    query_parts.append(queries_of(1))
    query_rows = query_parts[0] + query_parts[1]
    largest = None
    for m in range(blocks):
        slot = lax.broadcasted_iota(jnp.int32, (block_rows, HD), 0) + (m * block_rows) + base_slot
        total = scores[m * block_rows : (m + 1) * block_rows, :] + scores_of(query_parts[1], 1, m)
        total = jnp.where(slot < len_row, total, -jnp.inf)
        scores[m * block_rows : (m + 1) * block_rows, :] = total
        top = jnp.max(total, axis=0, keepdims=True)
        largest = top if largest is None else jnp.maximum(largest, top)
    others = own_other
    for k in range(1, dp):
        other_copies[k].wait_recv()
        others = others + other_in[k].astype(F32)
    new_keys = jnp.concatenate(
        [rms_rope(others[:, g * HD : (g + 1) * HD], k_gain[...], 0) for g in range(kv_heads)], axis=1
    ).astype(BF16)
    new_values = others[:, kv_cols:].astype(BF16)
    nk_out[...] = new_keys
    nv_out[...] = new_values

    own_scores = lax.dot_general(
        new_keys, jnp.concatenate([query_rows, query_rows], axis=0), contract_last, preferred_element_type=F32
    )
    own_lane = lax.broadcasted_iota(jnp.int32, (rows, HD), 1) % rows
    own_diag = lax.broadcasted_iota(jnp.int32, (rows, HD), 0) == own_lane
    own_row = jnp.sum(jnp.where(own_diag, own_scores, 0.0), axis=0, keepdims=True)
    largest = jnp.maximum(jnp.maximum(largest, pltpu.roll(largest, half_rows, 1)), own_row)
    own_weight = jnp.exp(own_row - largest)
    total_row = None
    for m in range(blocks):
        weight = jnp.exp(scores[m * block_rows : (m + 1) * block_rows, :] - largest)
        part_total = jnp.sum(weight, axis=0, keepdims=True)
        total_row = part_total if total_row is None else total_row + part_total
        probs[:, m * block_rows : (m + 1) * block_rows] = weight.T.astype(BF16)
    total_row = total_row + pltpu.roll(total_row, half_rows, 1) + own_weight
    eye = lax.broadcasted_iota(jnp.int32, (half_rows, HD), 0) == lax.broadcasted_iota(jnp.int32, (half_rows, HD), 1)
    total_col = jnp.sum(jnp.where(eye, total_row, 0.0), axis=1, keepdims=True)
    own_mix = jnp.where(own_diag, own_weight, 0.0)[:, :half_rows].astype(BF16)
    mixture = lax.dot_general(own_mix, new_values, (((0,), (0,)), ((), ())), preferred_element_type=F32)
    for copy in c_v:
        copy.wait()
    low_p = probs[:half_rows, :]
    high_p = probs[half_rows:, :]
    for b in range(rows):
        mixture = mixture + jnp.dot(low_p * picks[b], vcache[b, :slots_half, :], preferred_element_type=F32)
        mixture = mixture + jnp.dot(high_p * picks[b], vcache[b, slots_half:, :], preferred_element_type=F32)
    mixture = mixture / total_col
    attended = jnp.concatenate(
        [mixture[h * rows : (h + 1) * rows, (h // per_kv) * HD : (h // per_kv + 1) * HD] for h in range(heads)], axis=1
    ).astype(BF16)

    att_in[0] = attended
    third_copies = [None] * side
    for k in reversed(range(1, side)):
        third_copies[k] = send(
            att_in.at[0], att_in.at[k], s3.at[k], r3.at[k], {"dp": spread_peer(ring[k])}
        )
    for copy in late_copies:
        copy.wait_recv()
    for k in range(1, side):
        third_copies[k].wait_recv()
    products = lax.dot_general(
        att_in[...].reshape(side * rows, q_cols), oweight[...], contract_last, preferred_element_type=F32
    ).astype(BF16)

    for k in range(side):
        for t in range(tensor):
            first = k * rows + t * mine
            red_out[k, t] = products[first : first + mine, :]
    fourth_copies = []
    for k in reversed(range(side)):
        for turn, (step_z, step_c) in reversed(list(enumerate(line))):
            if k or turn:
                peer_t = line_peer((step_z, step_c))
                slot = red_in.at[my_c, place, step_z]
                fourth_copies.append(
                    send(
                        red_out.at[k, peer_t], slot, s4.at[k, turn], r4.at[k, turn],
                        {"dp": spread_peer(-ring[k] % side), "tensor": peer_t},
                    )
                )
    red_in[my_c, place, 0] = red_out[0, me_t]
    for copy in fourth_copies:
        copy.wait_recv()
    tiles = [jnp.zeros((mine, LANES), F32) for _ in range(width // LANES)]
    lane_pair = lax.broadcasted_iota(jnp.int32, (mine, LANES), 1)
    for d in range(dp):
        parts = []
        for c, p, a in ((0, d // side, d % side), (1, d % side, d // side)):
            for z in range(depth):
                parts.append(red_in[c, p, z, :, a * share_pad : (a + 1) * share_pad].astype(F32))
        while len(parts) > 1:
            parts = [parts[n] + parts[n + 1] for n in range(0, len(parts) - 1, 2)] + parts[len(parts) // 2 * 2 :]
        low, turn = share * d // LANES, share * d % LANES
        columns = [parts[0][:, n * LANES : (n + 1) * LANES] for n in range(share_pad // LANES)]
        if turn:
            columns = [pltpu.roll(column, turn, 1) for column in columns]
            none = jnp.zeros((mine, LANES), F32)
            columns = [
                jnp.where(lane_pair < turn, before, after)
                for before, after in zip([none] + columns, columns + [none])
            ]
        for n, column in enumerate(columns):
            if low + n < len(tiles) and n * LANES < turn + share:
                tiles[low + n] = tiles[low + n] + column
    square = tiles[0] * tiles[0]
    for tile in tiles[1:]:
        square = square + tile * tile
    scale = lax.rsqrt(jnp.sum(square, axis=1, keepdims=True) * (1.0 / width) + EPS)
    projected = jnp.concatenate(tiles, axis=1)
    row_out[...] = (tok_mine[...] + projected * scale * post_gain[...]).astype(BF16)

    keep = pltpu.make_async_copy(row_out, hid_hbm.at[me_t], last_sem)
    keep.start()
    fifth_copies = [
        send(row_out, hid_hbm.at[me_t], s5.at[k], r5.at[k], {"tensor": line_peer(line[k])})
        for k in reversed(range(1, tensor))
    ]
    for copy in sends:
        copy.wait_send()
    keep.wait()
    for copy in fifth_copies:
        copy.wait_recv()


def finish_kernel(hid_in, nk_in, nv_in, hid, nk, nv):
    hid[...] = hid_in[...].reshape(hid.shape)
    nk[...] = nk_in[...]
    nv[...] = nv_in[...]


def per_device(dp, tensor, side, *args):
    tokens, lengths, positions, in_gain, qw, kw, vw, q_gain, k_gain, kc, vc, ow, post_gain = args
    rows, width = tokens.shape
    share, q_cols = qw.shape
    kv_cols = kw.shape[1]
    ctx = kc.shape[1]
    share_pad = padded(share)
    cols = q_cols + 2 * kv_cols
    mine = rows // tensor
    depth = tensor // 2
    strip = side * share_pad
    dims = (dp, tensor, side, rows, width, share, q_cols, kv_cols, ctx, strip)
    exponent = np.arange(HD // 2, dtype=np.float64) * (2.0 / HD)
    frequency = (ROPE_BASE**-exponent).astype(np.float32)
    freq = jnp.asarray(np.concatenate([frequency, frequency])[None])
    any_spec = pl.BlockSpec(memory_space=pl.ANY)
    vmem_spec = pl.BlockSpec(memory_space=pltpu.VMEM)
    dma = pltpu.SemaphoreType.DMA
    hidden, new_keys, new_values = pl.pallas_call(
        functools.partial(kernel, dims),
        out_shape=(
            jax.ShapeDtypeStruct((tensor, mine, width), BF16),
            jax.ShapeDtypeStruct((rows, kv_cols), BF16),
            jax.ShapeDtypeStruct((rows, kv_cols), BF16),
        ),
        in_specs=[any_spec] * 14,
        out_specs=(any_spec, vmem_spec, vmem_spec),
        scratch_shapes=[
            pltpu.VMEM((rows, width), BF16),
            pltpu.VMEM((1, rows), jnp.int32),
            pltpu.VMEM((1, rows), jnp.int32),
            pltpu.VMEM((1, width), F32),
            pltpu.VMEM((share_pad, cols), BF16),
            pltpu.VMEM((1, HD), F32),
            pltpu.VMEM((1, HD), F32),
            pltpu.VMEM((rows, ctx, kv_cols), BF16),
            pltpu.VMEM((rows, ctx, kv_cols), BF16),
            pltpu.VMEM((strip, q_cols), BF16),
            pltpu.VMEM((1, width), F32),
            pltpu.VMEM((1, HD), F32),
            pltpu.VMEM((rows, width + 2 * LANES), F32),
            pltpu.VMEM((mine, width), F32),
            pltpu.VMEM((dp, rows, share_pad), BF16),
            pltpu.VMEM((dp, rows, share_pad), BF16),
            pltpu.VMEM((2, dp, rows // 2, q_cols), BF16),
            pltpu.VMEM((2, dp, rows // 2, q_cols), BF16),
            pltpu.VMEM((dp, rows, 2 * kv_cols), BF16),
            pltpu.VMEM((dp, rows, 2 * kv_cols), BF16),
            pltpu.VMEM((ctx // 2, HD), F32),
            pltpu.VMEM((HD, ctx // 2), BF16),
            pltpu.VMEM((side, rows, q_cols), BF16),
            pltpu.VMEM((side, tensor, mine, strip), BF16),
            pltpu.VMEM((2, side, depth, mine, strip), BF16),
            pltpu.VMEM((mine, width), BF16),
            dma((12,)),
            dma((2, rows)),
            dma((dp,)), dma((dp,)),
            dma((3, dp)), dma((3, dp)),
            dma((side,)), dma((side,)),
            dma((side, tensor)), dma((side, tensor)),
            dma((tensor,)), dma((tensor,)),
            dma((2, 3)), dma((2, 3)),
            dma(()),
        ],
        compiler_params=pltpu.CompilerParams(collective_id=0, has_side_effects=True, vmem_limit_bytes=50 * 1024 * 1024),
    )(
        *[
            pltpu.with_memory_space_constraint(operand, pltpu.HBM)
            for operand in (
                tokens, lengths.reshape(1, rows), positions.reshape(1, rows), in_gain, qw, kw, vw,
                q_gain.reshape(1, HD), k_gain.reshape(1, HD), kc, vc, ow.T, post_gain, freq,
            )
        ]
    )
    return pl.pallas_call(
        finish_kernel,
        out_shape=(
            jax.ShapeDtypeStruct((rows, width), BF16),
            jax.ShapeDtypeStruct((rows, kv_cols), BF16),
            jax.ShapeDtypeStruct((rows, kv_cols), BF16),
        ),
        compiler_params=pltpu.CompilerParams(vmem_limit_bytes=4 * 1024 * 1024),
    )(hidden, new_keys, new_values)


def solution(mesh):
    dp, tensor = mesh.shape["dp"], mesh.shape["tensor"]
    side = int(round(dp**0.5))
    return jax.shard_map(
        functools.partial(per_device, dp, tensor, side),
        mesh=mesh,
        in_specs=(
            P("dp", None), P("dp"), P("dp"), P(), P("dp", "tensor"), P("dp", "tensor"), P("dp", "tensor"), P(), P(),
            P("dp", None, "tensor"), P("dp", None, "tensor"), P("tensor", "dp"), P(),
        ),
        out_specs=(P("dp", None), P("dp", "tensor"), P("dp", "tensor")),
        check_vma=False,
    )
```
